256 devices in a mesh: sub: 32 (over y, z_hi, core), rng: 8 (over z_lo, x).
Axes of the slice: x: 4, y: 4, z: 8 (z_hi: 4, z_lo: 2; z = z_hi * 2 + z_lo), core: 2. Of those that a mesh axis runs over, the one named last changes fastest.
Arguments:
- image: bfloat16 [2, 8192, 4096], P(None, 'sub', 'rng'), may hold values from -30 to 30
- stencil: int32 [4, 2, 2, 256, 4], replicated, may hold values from 0 to 255, as said below
- interp_weights: float32 [4, 4], replicated, may hold values from 0.25 to 0.6
- range_taps: float32 [4, 2, 3], replicated, may hold values from 0.25 to 0.7
Outputs:
- merged: bfloat16 [2, 8192, 4096], P(None, 'sub', 'rng')
- beam_phase: float32 [2, 8192], P(None, 'sub')
The draws below stay inside these ranges and needn't reach their ends.
Inputs may be any that keep to these rules, and one draw needn't show every extreme that they name: `stencil`: for every section, half, child and beam the 4 indices are consecutive and rising.
All inputs are finite; a program needn't handle non-finite values.
Results may differ from the reference program's by a relative error of at most 0.012.
Values may be sent and summed in bfloat16 or wider, within the bound.
A program may use at most 64 MiB of HBM per device.

```python
import math
import jax
import jax.numpy as jnp
from jax import lax

ANG = 256
SECTIONS = 4
TAPS = 4
BEAMS = 8192
NR = 4096
N_SUB = 32


def draw_image(key, part):
    first_key = jax.random.fold_in(jax.random.fold_in(key, 11), 0)
    position = jnp.arange(NR, dtype=jnp.float32) / NR
    envelope = jnp.exp(position * math.log(3.0))
    values = jnp.clip(jax.random.normal(first_key, (2, BEAMS, NR), jnp.float32), -3.0, 3.0) * envelope
    return values.astype(jnp.bfloat16)


def draw_stencil(key, part):
    jitter = jax.random.randint(jax.random.fold_in(key, 5), (SECTIONS, 2, 2, ANG, 1), -2, 3)
    centre = (jnp.arange(2, dtype=jnp.int32)[:, None] * ANG + jnp.arange(ANG, dtype=jnp.int32)[None, :]) // 2
    start = jnp.clip(centre.reshape(1, 2, 1, ANG, 1) + jitter - 1, 0, ANG - TAPS)
    return (start + jnp.arange(TAPS, dtype=jnp.int32)).astype(jnp.int32)


def setup_inputs(seed: int = 0) -> dict:
    seeds = jax.random.split(jax.random.key(seed), 5)
    image = draw_image(jax.random.fold_in(seeds[4], 71), 0)
    stencil = draw_stencil(jax.random.fold_in(seeds[4], 71), 0)
    interp_weights = jnp.clip(jax.random.uniform(seeds[2], (SECTIONS, TAPS), jnp.float32, 0.25, 0.6), 0.25, 0.6)
    range_taps = jnp.clip(jax.random.uniform(seeds[3], (SECTIONS, 2, 3), jnp.float32, 0.25, 0.7), 0.25, 0.7)
    return dict(image=image, stencil=stencil, interp_weights=interp_weights, range_taps=range_taps)


epsilon = 1e-06

def coefficients(weights, section_num, beams_dev):
    beam_pos = jnp.arange(beams_dev, dtype=jnp.float32)
    half_pos = jnp.arange(2, dtype=jnp.float32).reshape(2, 1, 1)
    child_sign = (2.0 * jnp.arange(2, dtype=jnp.float32) - 1.0).reshape(1, 2, 1)
    angles = child_sign * (half_pos * beams_dev + beam_pos + 0.5) * (0.37 + 0.11 * section_num)
    weights = weights.astype(jnp.float32)
    real_part = (jnp.cos(angles)[..., None] * weights).astype(jnp.bfloat16)
    imag_part = (jnp.sin(angles)[..., None] * weights).astype(jnp.bfloat16)
    return (real_part, imag_part)

def rotate_rows(blocks, factors):
    values = blocks.astype(jnp.float32)
    real_factor = factors[0][..., None]
    imag_factor = factors[1][..., None]
    real_out = values[0] * real_factor - values[1] * imag_factor
    imag_out = values[0] * imag_factor + values[1] * real_factor
    return jnp.stack([real_out, imag_out]).astype(jnp.bfloat16)

def phase_factors(merged):
    values = merged.astype(jnp.float32)
    following = jnp.roll(values, -1, axis=2)
    lag_real = lax.optimization_barrier(jnp.sum(values[0] * following[0] + values[1] * following[1], axis=-1))
    lag_imag = lax.optimization_barrier(jnp.sum(values[0] * following[1] - values[1] * following[0], axis=-1))
    power = lax.optimization_barrier(jnp.sum((values[0] ** 2 + values[1] ** 2) * (following[0] ** 2 + following[1] ** 2), axis=-1))
    scale = 1.0 / jnp.sqrt(power + epsilon)
    return jnp.stack([lag_real * scale, -lag_imag * scale])

def reference(image, stencil, interp_weights, range_taps):
    blocks = image.reshape(2, N_SUB, ANG, NR)
    merged = blocks
    factors = None
    for section_num in range(SECTIONS):
        if section_num > 0:
            blocks = rotate_rows(merged, factors)
        real_part, imag_part = coefficients(interp_weights[section_num], section_num, ANG)
        span = 2 ** section_num
        source = blocks.astype(jnp.float32)

        def merge_block(block_num):
            half_bit = block_num // span % 2
            first = block_num - half_bit * span
            summed = jnp.zeros((2, ANG, NR), jnp.float32)
            for child_num in range(2):
                child = lax.dynamic_index_in_dim(source, first + child_num * span, 1, keepdims=False)
                indices = lax.dynamic_index_in_dim(stencil[section_num, :, child_num], half_bit, 0, keepdims=False)
                coef_re = lax.dynamic_index_in_dim(real_part[:, child_num], half_bit, 0, keepdims=False).astype(jnp.float32)
                coef_im = lax.dynamic_index_in_dim(imag_part[:, child_num], half_bit, 0, keepdims=False).astype(jnp.float32)
                picked = child[:, indices]
                part_re = lax.optimization_barrier(jnp.sum(coef_re[..., None] * picked[0] - coef_im[..., None] * picked[1], axis=1))
                part_im = lax.optimization_barrier(jnp.sum(coef_re[..., None] * picked[1] + coef_im[..., None] * picked[0], axis=1))
                padded = jnp.pad(jnp.stack([part_re, part_im]), ((0, 0), (0, 0), (1, 1)))
                for tap_num in range(3):
                    summed = summed + range_taps[section_num, child_num, tap_num] * padded[:, :, tap_num:tap_num + NR]
            return summed.astype(jnp.bfloat16)
        merged = lax.map(merge_block, jnp.arange(N_SUB, dtype=jnp.int32))
        merged = jnp.transpose(merged, (1, 0, 2, 3))
        factors = phase_factors(merged)
    return (merged.reshape(2, BEAMS, NR), factors.reshape(2, BEAMS))
```

```python
import functools

import jax
import jax.numpy as jnp
import numpy as np
from jax import lax
from jax.experimental import pallas as pl
from jax.experimental.pallas import tpu as pltpu
from jax.sharding import PartitionSpec as P

SECTIONS = 4
TAPS = 4
EPS = 1e-6
MESH = pl.DeviceIdType.MESH
F32 = jnp.float32
BF16 = jnp.bfloat16


def angle_tables(beams):
    rows = []
    for s in range(SECTIONS):
        for h in range(2):
            for c in range(2):
                pos = np.float32(h * beams) + np.arange(beams, dtype=np.float32) + np.float32(0.5)
                rows.append(np.float32(2 * c - 1) * pos * np.float32(0.37 + 0.11 * s))
    psi = np.stack(rows).astype(np.float64)
    return np.cos(psi).astype(np.float32), np.sin(psi).astype(np.float32)


def kernel(
    n_rng,
    weights,
    taps,
    image,
    start,
    cosines,
    sines,
    merged,
    phase,
    own,
    got,
    matrix,
    acc0,
    acc1,
    acc2,
    prod,
    edge_out,
    edge_in,
    sums_out,
    sums_in,
    fac_out,
    fac_in,
    bulk_send,
    bulk_recv,
    edge_send,
    edge_recv,
    rim_send,
    rim_recv,
    sums_send,
    sums_recv,
    fac_send,
    fac_recv,
):
    sub = lax.axis_index("sub")
    rho = lax.axis_index("rng")
    beams = image.shape[1]
    rows = image.shape[2]
    total = rows + 16
    step = 128
    chunks = rows // step
    halves = [lax.rem(sub // 2**s, 2) for s in range(SECTIONS)]
    partners = [sub + 2**s * (1 - 2 * halves[s]) for s in range(SECTIONS)]
    peers = [lax.rem(rho + d, n_rng) for d in range(1, n_rng)]

    barrier = pltpu.get_barrier_semaphore()
    for s in range(SECTIONS):
        pl.semaphore_signal(barrier, inc=1, device_id=(partners[s], rho), device_id_type=MESH)
    for peer in peers:
        pl.semaphore_signal(barrier, inc=1, device_id=(sub, peer), device_id_type=MESH)

    def build(s):
        for which in range(2):
            half = halves[s]
            child = half if which == 0 else 1 - half
            row = s * 4 + half * 2 + child
            shift = lax.broadcasted_iota(jnp.int32, (beams, beams), 0) - start[pl.ds(row, 1), :]
            cos_row = cosines[pl.ds(row, 1), :]
            sin_row = sines[pl.ds(row, 1), :]
            real = jnp.zeros((beams, beams), F32)
            imag = jnp.zeros((beams, beams), F32)
            for t in range(TAPS):
                hit = shift == t
                real = jnp.where(hit, cos_row * weights[s * TAPS + t], real)
                imag = jnp.where(hit, sin_row * weights[s * TAPS + t], imag)
            matrix[s, which, 0:beams, 0:beams] = real.astype(BF16)
            matrix[s, which, 0:beams, beams : 2 * beams] = imag.astype(BF16)
            matrix[s, which, beams : 2 * beams, 0:beams] = (-imag).astype(BF16)
            matrix[s, which, beams : 2 * beams, beams : 2 * beams] = real.astype(BF16)

    for j in range(chunks):
        for part in range(2):
            block = image[part, :, j * step : (j + 1) * step].astype(F32)
            own[0, j * step : (j + 1) * step, part * beams : (part + 1) * beams] = block.T.astype(BF16)
    first = own[0, 0:16, :].astype(F32)
    last = own[0, rows - 16 : rows, :].astype(F32)
    edge_out[...] = jnp.concatenate([first[0:8], last[8:16]], axis=0).astype(BF16)

    pl.semaphore_wait(barrier, SECTIONS + n_rng - 1)

    def bulk(s):
        if s == 0:
            return pltpu.make_async_remote_copy(
                src_ref=own.at[0, pl.ds(0, rows)],
                dst_ref=got.at[0, pl.ds(0, rows)],
                send_sem=bulk_send.at[0],
                recv_sem=bulk_recv.at[0],
                device_id=(partners[0], rho),
                device_id_type=MESH,
            )
        return pltpu.make_async_remote_copy(
            src_ref=own.at[s],
            dst_ref=got.at[s],
            send_sem=bulk_send.at[s],
            recv_sem=bulk_recv.at[s],
            device_id=(partners[s], rho),
            device_id_type=MESH,
        )

    below, above = lax.rem(rho + n_rng - 1, n_rng), lax.rem(rho + 1, n_rng)

    def edge(side):
        return pltpu.make_async_remote_copy(
            src_ref=edge_out,
            dst_ref=edge_in.at[side],
            send_sem=edge_send.at[side],
            recv_sem=edge_recv.at[side],
            device_id=(sub, above if side == 0 else below),
            device_id_type=MESH,
        )

    rim = pltpu.make_async_remote_copy(
        src_ref=own.at[0, pl.ds(rows, 16)],
        dst_ref=got.at[0, pl.ds(rows, 16)],
        send_sem=rim_send.at[0],
        recv_sem=rim_recv.at[0],
        device_id=(partners[0], rho),
        device_id_type=MESH,
    )

    edge(0).start()
    edge(1).start()
    bulk(0).start()
    build(0)

    row_id = lax.broadcasted_iota(jnp.int32, (16, 2 * beams), 0)
    low = jnp.where(rho < n_rng - 1, 1.0, 0.0).astype(F32)
    high = jnp.where(rho > 0, 1.0, 0.0).astype(F32)
    mask = jnp.where(row_id < 8, low, high)

    edge(0).wait()
    edge(1).wait()
    halo = jnp.concatenate([edge_in[1].astype(F32)[0:8], edge_in[0].astype(F32)[8:16]], axis=0)
    own[0, rows:total, :] = (halo * mask).astype(BF16)
    rim.start()
    build(1)

    def rotated(ref, s, base, size, factor):
        value = ref[s, pl.ds(base, size), :]
        if factor is None:
            return value
        value = value.astype(F32)
        real, imag = value[:, :beams], value[:, beams:]
        g_re, g_im = factor
        return jnp.concatenate(
            [(real * g_re - imag * g_im).astype(BF16), (real * g_im + imag * g_re).astype(BF16)], axis=1
        )

    big = total // 3

    for s in range(SECTIONS):
        half = halves[s]
        if s == 0:
            own_factor = got_factor = None
        else:
            own_factor = (fac_out[s - 1, 0:1, :], fac_out[s - 1, 1:2, :])

        @pl.loop(0, 3)
        def _(i, s=s, factor=own_factor):
            base = pl.multiple_of(i * big, 16)
            prod[pl.ds(base, big), :] = jnp.dot(
                rotated(own, s, base, big, factor), matrix[s, 0], preferred_element_type=F32
            )

        if s == 0:
            rim.wait_recv()
        else:
            if s + 1 < SECTIONS:
                build(s + 1)
            factor_copy(s - 1).wait_recv()
            got_factor = (fac_in[s - 1, 0:1, :], fac_in[s - 1, 1:2, :])
        bulk(s).wait_recv()
        own_taps = [taps[s * 6 + half * 3 + k] for k in range(3)]
        got_taps = [taps[s * 6 + (1 - half) * 3 + k] for k in range(3)]

        @pl.loop(0, 3)
        def _(i, s=s, factor=got_factor, own_taps=own_taps, got_taps=got_taps):
            base = pl.multiple_of(i * big, 16)
            theirs = jnp.dot(rotated(got, s, base, big, factor), matrix[s, 1], preferred_element_type=F32)
            mine = prod[pl.ds(base, big), :]
            acc0[pl.ds(base + 8, big), :] = own_taps[0] * mine + got_taps[0] * theirs
            acc1[pl.ds(base, big), :] = own_taps[1] * mine + got_taps[1] * theirs
            acc2[pl.ds(base, big), :] = own_taps[2] * mine + got_taps[2] * theirs

        acc0[0:8, :] = acc0[total : total + 8, :]
        acc2[total : total + 8, :] = acc2[0:8, :]

        def merge(base, size):
            lower = acc0[pl.ds(base, size + 8), :][7 : 7 + size]
            upper = acc2[pl.ds(base, size + 8), :][1 : 1 + size]
            return acc1[pl.ds(base, size), :] + lower + upper

        sums = [jnp.zeros((8, beams), F32) for _ in range(3)]

        def tally(y, sums):
            real, imag = y[:, :beams], y[:, beams:]
            real_next, imag_next = pltpu.roll(real, beams - 1, 1), pltpu.roll(imag, beams - 1, 1)
            size = real.shape[0]
            terms = (
                real * real_next + imag * imag_next,
                real * imag_next - imag * real_next,
                (real * real + imag * imag) * (real_next * real_next + imag_next * imag_next),
            )
            return [
                a + jnp.sum(term.reshape(size // 8, 8, beams), axis=0) for a, term in zip(sums, terms)
            ]

        if s < SECTIONS - 1:
            piece = 64

            def body(i, sums, s=s):
                base = pl.multiple_of(i * piece, piece)
                y = merge(base, piece).astype(BF16)
                own[s + 1, pl.ds(base, piece), :] = y
                return tally(y.astype(F32), sums)

            sums = lax.fori_loop(0, rows // piece, body, sums)
            own[s + 1, rows:total, :] = (merge(rows, 16) * mask).astype(BF16)
        else:
            for j in range(chunks):
                y = merge(j * step, step).astype(BF16).astype(F32)
                for part in range(2):
                    merged[part, :, j * step : (j + 1) * step] = (
                        y[:, part * beams : (part + 1) * beams].T.astype(BF16)
                    )
                sums = tally(y, sums)

        line = lax.broadcasted_iota(jnp.int32, (8, beams), 0)
        packed = jnp.zeros((8, beams), F32)
        for k in range(3):
            packed = jnp.where(line == k, jnp.sum(sums[k], axis=0, keepdims=True), packed)
        sums_out[s] = packed
        sums_in[s, rho] = packed

        def sums_copy(d, s=s):
            return pltpu.make_async_remote_copy(
                src_ref=sums_out.at[s],
                dst_ref=sums_in.at[s, rho],
                send_sem=sums_send.at[s, d],
                recv_sem=sums_recv.at[s, d],
                device_id=(sub, peers[d]),
                device_id_type=MESH,
            )

        def sums_arrived(d, s=s):
            return pltpu.make_async_remote_copy(
                src_ref=sums_out.at[s],
                dst_ref=sums_in.at[s, peers[n_rng - 2 - d]],
                send_sem=sums_send.at[s, d],
                recv_sem=sums_recv.at[s, d],
                device_id=(sub, peers[d]),
                device_id_type=MESH,
            )

        for d in range(n_rng - 1):
            sums_copy(d).start()
        if s < SECTIONS - 1:
            bulk(s + 1).start()
        for d in range(n_rng - 1):
            sums_arrived(d).wait_recv()
        full = sums_in[s, 0]
        for other in range(1, n_rng):
            full = full + sums_in[s, other]
        scale = 1.0 / jnp.sqrt(full[2:3] + EPS)
        g_re, g_im = full[0:1] * scale, -(full[1:2] * scale)
        if s < SECTIONS - 1:
            fac_out[s] = jnp.where(line == 0, g_re, jnp.where(line == 1, g_im, 0.0))

            def factor_copy(s):
                return pltpu.make_async_remote_copy(
                    src_ref=fac_out.at[s],
                    dst_ref=fac_in.at[s],
                    send_sem=fac_send.at[s],
                    recv_sem=fac_recv.at[s],
                    device_id=(partners[s + 1], rho),
                    device_id_type=MESH,
                )

            factor_copy(s).start()
        else:
            phase[0:1, :] = g_re
            phase[1:2, :] = g_im

    rim.wait_send()
    for s in range(SECTIONS):
        bulk(s).wait_send()
        for d in range(n_rng - 1):
            pltpu.make_async_remote_copy(
                src_ref=sums_out.at[s],
                dst_ref=sums_in.at[s, rho],
                send_sem=sums_send.at[s, d],
                recv_sem=sums_recv.at[s, d],
                device_id=(sub, peers[d]),
                device_id_type=MESH,
            ).wait_send()
        if s < SECTIONS - 1:
            factor_copy(s).wait_send()


def solution(mesh):
    n_rng = mesh.shape["rng"]

    def on_device(image, stencil, interp_weights, range_taps):
        _, beams, rows = image.shape
        total = rows + 16
        cosines, sines = angle_tables(beams)
        start = stencil[..., 0].reshape(SECTIONS * 4, beams)
        vmem = pl.BlockSpec(memory_space=pltpu.VMEM)
        smem = pl.BlockSpec(memory_space=pltpu.SMEM)
        dma = pltpu.SemaphoreType.DMA
        return pl.pallas_call(
            functools.partial(kernel, n_rng),
            out_shape=(
                jax.ShapeDtypeStruct((2, beams, rows), BF16),
                jax.ShapeDtypeStruct((2, beams), F32),
            ),
            in_specs=[smem, smem, vmem, vmem, vmem, vmem],
            out_specs=(vmem, vmem),
            scratch_shapes=[
                pltpu.VMEM((SECTIONS, total, 2 * beams), BF16),
                pltpu.VMEM((SECTIONS, total, 2 * beams), BF16),
                pltpu.VMEM((SECTIONS, 2, 2 * beams, 2 * beams), BF16),
                pltpu.VMEM((total + 8, 2 * beams), F32),
                pltpu.VMEM((total, 2 * beams), F32),
                pltpu.VMEM((total + 8, 2 * beams), F32),
                pltpu.VMEM((total, 2 * beams), F32),
                pltpu.VMEM((16, 2 * beams), BF16),
                pltpu.VMEM((2, 16, 2 * beams), BF16),
                pltpu.VMEM((SECTIONS, 8, beams), F32),
                pltpu.VMEM((SECTIONS, n_rng, 8, beams), F32),
                pltpu.VMEM((SECTIONS - 1, 8, beams), F32),
                pltpu.VMEM((SECTIONS - 1, 8, beams), F32),
                dma((SECTIONS,)),
                dma((SECTIONS,)),
                dma((2,)),
                dma((2,)),
                dma((1,)),
                dma((1,)),
                dma((SECTIONS, n_rng - 1)),
                dma((SECTIONS, n_rng - 1)),
                dma((SECTIONS - 1,)),
                dma((SECTIONS - 1,)),
            ],
            compiler_params=pltpu.CompilerParams(
                collective_id=0, has_side_effects=True, vmem_limit_bytes=48 * 1024 * 1024
            ),
        )(
            interp_weights.reshape(-1),
            range_taps.reshape(-1),
            image,
            start,
            jnp.asarray(cosines),
            jnp.asarray(sines),
        )

    return jax.shard_map(
        on_device,
        mesh=mesh,
        in_specs=(P(None, "sub", "rng"), P(), P(), P()),
        out_specs=(P(None, "sub", "rng"), P(None, "sub")),
        check_vma=False,
    )
```

```python
import functools

import jax
import jax.numpy as jnp
import numpy as np
from jax import lax
from jax.experimental import pallas as pl
from jax.experimental.pallas import tpu as pltpu
from jax.sharding import PartitionSpec as P

SECTIONS = 4
TAPS = 4
EPS = 1e-6
STEP = 128
EARLY = [lambda k: 0, lambda k: 0, lambda k: k - 3, lambda k: 0]
MIDDLE = [lambda k: 3, lambda k: 2, lambda k: k, lambda k: 0]
MESH = pl.DeviceIdType.MESH
F32 = jnp.float32
BF16 = jnp.bfloat16


def angle_tables(beams):
    rows = []
    for s in range(SECTIONS):
        for h in range(2):
            for c in range(2):
                pos = np.float32(h * beams) + np.arange(beams, dtype=np.float32) + np.float32(0.5)
                rows.append(np.float32(2 * c - 1) * pos * np.float32(0.37 + 0.11 * s))
    psi = np.stack(rows).astype(np.float64)
    return np.cos(psi).astype(np.float32), np.sin(psi).astype(np.float32)


def plan(order, n):
    done, out = set(), []
    groups = []
    for piece in order:
        done.add(piece)
        ready = [
            p
            for p in [n] + list(range(n))
            if p not in out and {p, (p + 1) % (n + 1), (p - 1) % (n + 1)} <= done
        ]
        out += ready
        groups.append(ready)
    return groups, out


def kernel(
    n_rng,
    weights,
    taps,
    image_hbm,
    stencil_hbm,
    trig_hbm,
    merged,
    phase,
    image,
    stencil,
    trig,
    own,
    got,
    matrix,
    acc0,
    acc1,
    acc2,
    prod,
    edge_out,
    edge_in,
    sums_out,
    sums_in,
    sums_far,
    fac_out,
    fac_in,
    load_sem,
    bulk_send,
    bulk_recv,
    edge_send,
    edge_recv,
    sums_send,
    sums_recv,
    far_send,
    far_recv,
    fac_send,
    fac_recv,
):
    sub = lax.axis_index("sub")
    rho = lax.axis_index("rng")
    beams = image.shape[1]
    rows = image.shape[2]
    total = rows + 16
    n = rows // STEP
    last = SECTIONS - 1
    halves = [lax.rem(sub // 2**s, 2) for s in range(SECTIONS)]
    partners = [sub + 2**s * (1 - 2 * halves[s]) for s in range(SECTIONS)]
    peers = [lax.rem(rho + d, n_rng) for d in range(1, n_rng)]

    barrier = pltpu.get_barrier_semaphore()
    for s in range(SECTIONS):
        pl.semaphore_signal(barrier, inc=1, device_id=(partners[s], rho), device_id_type=MESH)
    for peer in peers:
        pl.semaphore_signal(barrier, inc=1, device_id=(sub, peer), device_id_type=MESH)
        pl.semaphore_signal(barrier, inc=1, device_id=(partners[last], peer), device_id_type=MESH)

    loads = [
        pltpu.make_async_copy(image_hbm, image, load_sem.at[0]),
        pltpu.make_async_copy(stencil_hbm, stencil, load_sem.at[1]),
        pltpu.make_async_copy(trig_hbm, trig, load_sem.at[2]),
    ]
    for load in loads:
        load.start()

    def build(s):
        for which in range(2):
            half = halves[s]
            child = half if which == 0 else 1 - half
            row = s * 4 + half * 2 + child
            shift = lax.broadcasted_iota(jnp.int32, (beams, beams), 0) - stencil[row, 0:1, :]
            cos_row = trig[0, pl.ds(row, 1), :]
            sin_row = trig[1, pl.ds(row, 1), :]
            real = jnp.zeros((beams, beams), F32)
            imag = jnp.zeros((beams, beams), F32)
            for t in range(TAPS):
                hit = shift == t
                real = jnp.where(hit, cos_row * weights[s, t], real)
                imag = jnp.where(hit, sin_row * weights[s, t], imag)
            matrix[s, which, 0:beams, 0:beams] = real.astype(BF16)
            matrix[s, which, 0:beams, beams : 2 * beams] = imag.astype(BF16)
            matrix[s, which, beams : 2 * beams, 0:beams] = (-imag).astype(BF16)
            matrix[s, which, beams : 2 * beams, beams : 2 * beams] = real.astype(BF16)

    for load in loads:
        load.wait()
    for j in range(rows // 128):
        for part in range(2):
            block = image[part, :, j * 128 : (j + 1) * 128].astype(F32)
            own[0, j * 128 : (j + 1) * 128, part * beams : (part + 1) * beams] = block.T.astype(BF16)
    low_edge = own[0, 0:16, :].astype(F32)
    high_edge = own[0, rows - 16 : rows, :].astype(F32)
    edge_out[...] = jnp.concatenate([low_edge[0:8], high_edge[8:16]], axis=0).astype(BF16)

    pl.semaphore_wait(barrier, SECTIONS + 2 * (n_rng - 1))

    def span(piece):
        return (rows, 16) if piece == n else (piece * STEP, STEP)

    def bulk(s, piece):
        base, size = (0, rows) if s == 0 and piece == 0 else span(piece)
        return pltpu.make_async_remote_copy(
            src_ref=own.at[s, pl.ds(base, size)],
            dst_ref=got.at[s, pl.ds(base, size)],
            send_sem=bulk_send.at[s, piece],
            recv_sem=bulk_recv.at[s, piece],
            device_id=(partners[s], rho),
            device_id_type=MESH,
        )

    below, above = lax.rem(rho + n_rng - 1, n_rng), lax.rem(rho + 1, n_rng)

    def edge(side):
        return pltpu.make_async_remote_copy(
            src_ref=edge_out,
            dst_ref=edge_in.at[side],
            send_sem=edge_send.at[side],
            recv_sem=edge_recv.at[side],
            device_id=(sub, above if side == 0 else below),
            device_id_type=MESH,
        )

    edge(0).start()
    edge(1).start()
    bulk(0, 0).start()
    build(0)

    row_id = lax.broadcasted_iota(jnp.int32, (16, 2 * beams), 0)
    low = jnp.where(rho < n_rng - 1, 1.0, 0.0).astype(F32)
    high = jnp.where(rho > 0, 1.0, 0.0).astype(F32)
    mask = jnp.where(row_id < 8, low, high)

    edge(0).wait()
    edge(1).wait()
    halo = jnp.concatenate([edge_in[1].astype(F32)[0:8], edge_in[0].astype(F32)[8:16]], axis=0)
    own[0, rows:total, :] = (halo * mask).astype(BF16)
    bulk(0, n).start()

    def rotated(ref, s, base, size, factor):
        value = ref[s, pl.ds(base, size), :]
        if factor is None:
            return value
        value = value.astype(F32)
        real, imag = value[:, :beams], value[:, beams:]
        g_re, g_im = factor
        return jnp.concatenate(
            [(real * g_re - imag * g_im).astype(BF16), (real * g_im + imag * g_re).astype(BF16)], axis=1
        )

    def gathered(ref, slot):
        full = ref[slot, 0]
        for other in range(1, n_rng):
            full = full + ref[slot, other]
        scale = 1.0 / jnp.sqrt(full[2:3] + EPS)
        return full[0:1] * scale, -(full[1:2] * scale)

    def merge(base, size):
        lower = acc0[base : base + size + 8, :][7 : 7 + size]
        upper = acc2[base : base + size + 8, :][1 : 1 + size]
        return acc1[base : base + size, :] + lower + upper

    def tally(y, sums):
        real, imag = y[:, :beams], y[:, beams:]
        real_next, imag_next = pltpu.roll(real, beams - 1, 1), pltpu.roll(imag, beams - 1, 1)
        size = real.shape[0]
        terms = (
            real * real_next + imag * imag_next,
            real * imag_next - imag * real_next,
            (real * real + imag * imag) * (real_next * real_next + imag_next * imag_next),
        )
        return [a + jnp.sum(term.reshape(size // 8, 8, beams), axis=0) for a, term in zip(sums, terms)]

    def sums_copy(s, d, slot):
        return pltpu.make_async_remote_copy(
            src_ref=sums_out.at[s],
            dst_ref=sums_in.at[s, slot],
            send_sem=sums_send.at[s, d],
            recv_sem=sums_recv.at[s, d],
            device_id=(sub, peers[d]),
            device_id_type=MESH,
        )

    def far_copy(d, slot):
        return pltpu.make_async_remote_copy(
            src_ref=sums_out.at[last - 1],
            dst_ref=sums_far.at[0, slot],
            send_sem=far_send.at[d],
            recv_sem=far_recv.at[d],
            device_id=(partners[last], rho if d == n_rng - 1 else peers[d]),
            device_id_type=MESH,
        )

    def factor_copy(s):
        return pltpu.make_async_remote_copy(
            src_ref=fac_out.at[s],
            dst_ref=fac_in.at[s],
            send_sem=fac_send.at[s],
            recv_sem=fac_recv.at[s],
            device_id=(partners[s + 1], rho),
            device_id_type=MESH,
        )

    line = lax.broadcasted_iota(jnp.int32, (8, beams), 0)
    big = total // 3
    order = [0, n]
    own_factor = got_factor = None

    for s in range(SECTIONS):
        half = halves[s]

        @pl.loop(0, 3)
        def _(i, s=s, factor=own_factor):
            base = pl.multiple_of(i * big, 16)
            prod[pl.ds(base, big), :] = jnp.dot(
                rotated(own, s, base, big, factor), matrix[s, 0], preferred_element_type=F32
            )

        if s < last:
            build(s + 1)
        if 0 < s < last:
            factor_copy(s - 1).wait_recv()
            got_factor = (fac_in[s - 1, 0:1, :], fac_in[s - 1, 1:2, :])
        own_taps = [taps[k, half, s] for k in range(3)]
        got_taps = [taps[k, 1 - half, s] for k in range(3)]

        def combine(base, size, s=s, factor=got_factor, own_taps=own_taps, got_taps=got_taps):
            theirs = jnp.dot(rotated(got, s, base, size, factor), matrix[s, 1], preferred_element_type=F32)
            mine = prod[pl.ds(base, size), :]
            acc0[pl.ds(base + 8, size), :] = own_taps[0] * mine + got_taps[0] * theirs
            acc1[pl.ds(base, size), :] = own_taps[1] * mine + got_taps[1] * theirs
            acc2[pl.ds(base, size), :] = own_taps[2] * mine + got_taps[2] * theirs

        sums = [jnp.zeros((8, beams), F32) for _ in range(3)]
        if s == 0:
            bulk(0, 0).wait_recv()
            bulk(0, n).wait_recv()

            @pl.loop(0, 3)
            def _(i):
                combine(pl.multiple_of(i * big, 16), big)

            acc0[0:8, :] = acc0[total : total + 8, :]
            acc2[total : total + 8, :] = acc2[0:8, :]
            groups, produced = [[n] + list(range(n))], [n] + list(range(n))
        else:
            groups, produced = plan(order, n)
        if s == last:
            bulk(0, 0).wait_send()
            bulk(0, n).wait_send()
        early, middle = EARLY[s](len(produced)), MIDDLE[s](len(produced))
        sent = 0
        for g, group in enumerate(groups):
            if s > 0:
                piece = order[g]
                bulk(s, piece).wait_recv()
                base, size = span(piece)
                combine(base, size)
                if piece == n:
                    acc0[0:8, :] = acc0[total : total + 8, :]
                if piece == 0:
                    acc2[total : total + 8, :] = acc2[0:8, :]
            for piece in group:
                base, size = span(piece)
                if s == last:
                    if piece == n:
                        continue
                    y = merge(base, size).astype(BF16)
                    own[0, base : base + size, :] = y
                    sums = tally(y.astype(F32), sums)
                    continue
                if piece == n:
                    own[s + 1, rows:total, :] = (merge(rows, 16) * mask).astype(BF16)
                else:
                    y = merge(base, size).astype(BF16)
                    own[s + 1, base : base + size, :] = y
                    sums = tally(y.astype(F32), sums)
                if sent < early:
                    bulk(s + 1, piece).start()
                    sent += 1

        packed = jnp.zeros((8, beams), F32)
        for k in range(3):
            packed = jnp.where(line == k, jnp.sum(sums[k], axis=0, keepdims=True), packed)
        sums_out[s] = packed
        sums_in[s, rho] = packed
        for d in range(n_rng - 1):
            sums_copy(s, d, rho).start()
        if s == last - 1:
            for d in range(n_rng):
                far_copy(d, rho).start()
        if s < last:
            while sent < middle:
                bulk(s + 1, produced[sent]).start()
                sent += 1
        else:
            for j in range(rows // 128):
                y = own[0, j * 128 : (j + 1) * 128, :].astype(F32)
                for part in range(2):
                    merged[part, :, j * 128 : (j + 1) * 128] = (
                        y[:, part * beams : (part + 1) * beams].T.astype(BF16)
                    )
        for d in range(n_rng - 1):
            sums_copy(s, d, peers[n_rng - 2 - d]).wait_recv()
        g_re, g_im = gathered(sums_in, s)
        if s < last:
            own_factor = (g_re, g_im)
            if s < last - 1:
                fac_out[s] = jnp.where(line == 0, g_re, jnp.where(line == 1, g_im, 0.0))
                factor_copy(s).start()
            while sent < len(produced):
                bulk(s + 1, produced[sent]).start()
                sent += 1
            if s == last - 1:
                for d in range(n_rng - 1):
                    far_copy(d, peers[n_rng - 2 - d]).wait_recv()
                far_copy(n_rng - 1, rho).wait_recv()
                got_factor = gathered(sums_far, 0)
        else:
            phase[0:1, :] = g_re
            phase[1:2, :] = g_im
        order = produced

    for s in range(SECTIONS):
        if s > 0:
            for piece in range(n + 1):
                bulk(s, piece).wait_send()
        for d in range(n_rng - 1):
            sums_copy(s, d, rho).wait_send()
        if s < last - 1:
            factor_copy(s).wait_send()
    for d in range(n_rng):
        far_copy(d, rho).wait_send()


def solution(mesh):
    n_rng = mesh.shape["rng"]

    def on_device(image, stencil, interp_weights, range_taps):
        _, beams, rows = image.shape
        total = rows + 16
        cosines, sines = angle_tables(beams)
        pieces = rows // STEP + 1
        hbm = pl.BlockSpec(memory_space=pltpu.HBM)
        vmem = pl.BlockSpec(memory_space=pltpu.VMEM)
        smem = pl.BlockSpec(memory_space=pltpu.SMEM)
        dma = pltpu.SemaphoreType.DMA
        return pl.pallas_call(
            functools.partial(kernel, n_rng),
            out_shape=(
                jax.ShapeDtypeStruct((2, beams, rows), BF16),
                jax.ShapeDtypeStruct((2, beams), F32),
            ),
            in_specs=[smem, smem, hbm, hbm, hbm],
            out_specs=(vmem, vmem),
            scratch_shapes=[
                pltpu.VMEM((2, beams, rows), BF16),
                pltpu.VMEM((SECTIONS * 4, TAPS, beams), jnp.int32),
                pltpu.VMEM((2, SECTIONS * 4, beams), F32),
                pltpu.VMEM((SECTIONS, total, 2 * beams), BF16),
                pltpu.VMEM((SECTIONS, total, 2 * beams), BF16),
                pltpu.VMEM((SECTIONS, 2, 2 * beams, 2 * beams), BF16),
                pltpu.VMEM((total + 8, 2 * beams), F32),
                pltpu.VMEM((total, 2 * beams), F32),
                pltpu.VMEM((total + 8, 2 * beams), F32),
                pltpu.VMEM((total, 2 * beams), F32),
                pltpu.VMEM((16, 2 * beams), BF16),
                pltpu.VMEM((2, 16, 2 * beams), BF16),
                pltpu.VMEM((SECTIONS, 8, beams), F32),
                pltpu.VMEM((SECTIONS, n_rng, 8, beams), F32),
                pltpu.VMEM((1, n_rng, 8, beams), F32),
                pltpu.VMEM((SECTIONS - 2, 8, beams), F32),
                pltpu.VMEM((SECTIONS - 2, 8, beams), F32),
                dma((3,)),
                dma((SECTIONS, pieces)),
                dma((SECTIONS, pieces)),
                dma((2,)),
                dma((2,)),
                dma((SECTIONS, n_rng - 1)),
                dma((SECTIONS, n_rng - 1)),
                dma((n_rng,)),
                dma((n_rng,)),
                dma((SECTIONS - 2,)),
                dma((SECTIONS - 2,)),
            ],
            compiler_params=pltpu.CompilerParams(
                collective_id=0, has_side_effects=True, vmem_limit_bytes=67043328
            ),
        )(
            interp_weights,
            range_taps.transpose(2, 1, 0),
            image,
            stencil.transpose(0, 1, 2, 4, 3).reshape(SECTIONS * 4, TAPS, beams),
            jnp.asarray(np.stack([cosines, sines])),
        )

    return jax.shard_map(
        on_device,
        mesh=mesh,
        in_specs=(P(None, "sub", "rng"), P(), P(), P()),
        out_specs=(P(None, "sub", "rng"), P(None, "sub")),
        check_vma=False,
    )
```

```python
import functools

import jax
import jax.numpy as jnp
import numpy as np
from jax import lax
from jax.experimental import pallas as pl
from jax.experimental.pallas import tpu as pltpu
from jax.sharding import PartitionSpec as P

SECTIONS = 4
TAPS = 4
EPS = 1e-6
QUARTERS = 4
CHUNK = 128
WITH_RIM = CHUNK + 16
MESH = pl.DeviceIdType.MESH
F32 = jnp.float32
BF16 = jnp.bfloat16


def angle_tables(beams):
    rows = []
    for s in range(SECTIONS):
        for h in range(2):
            for c in range(2):
                pos = np.float32(h * beams) + np.arange(beams, dtype=np.float32) + np.float32(0.5)
                rows.append(np.float32(2 * c - 1) * pos * np.float32(0.37 + 0.11 * s))
    psi = np.stack(rows).astype(np.float64)
    return np.cos(psi).astype(np.float32), np.sin(psi).astype(np.float32)


def kernel(
    n_rng,
    weights,
    taps,
    image_hbm,
    stencil_hbm,
    trig_hbm,
    merged,
    phase,
    image,
    stencil,
    trig,
    own,
    got,
    matrix,
    acc0,
    acc1,
    acc2,
    prod,
    edge_out,
    edge_in,
    sums_out,
    sums_in,
    split_out,
    split_in,
    stacked,
    terms,
    middle_y,
    back_out,
    back_in,
    far_in,
    fac_out,
    fac_in,
    far_fac_out,
    far_fac_in,
    wide_out,
    wide_in,
    part_out,
    part_in,
    load_sem,
    core_send,
    core_recv,
    edge_send,
    edge_recv,
    sums_send,
    sums_recv,
    split_send,
    split_recv,
    back_send,
    back_recv,
    far_send,
    far_recv,
    fac_send,
    fac_recv,
    wide_send,
    wide_recv,
    part_send,
    part_recv,
):
    sub = lax.axis_index("sub")
    rho = lax.axis_index("rng")
    beams = image.shape[1]
    rows = image.shape[2]
    total = rows + 16
    width = 2 * beams
    quarter = lax.rem(sub // 2, QUARTERS)
    core_half = lax.rem(sub, 2)
    y_half = lax.rem(sub // 8, 2)
    core_partner = sub + 1 - 2 * core_half
    y_partner = sub + 8 * (1 - 2 * y_half)
    ahead = [lax.rem(quarter + e, QUARTERS) for e in range(QUARTERS)]
    behind = [lax.rem(quarter + QUARTERS - e, QUARTERS) for e in range(QUARTERS)]
    peers = [lax.rem(rho + d, n_rng) for d in range(1, n_rng)]

    def at_quarter(other):
        return sub + 2 * (other - quarter)

    barrier = pltpu.get_barrier_semaphore()
    for other in (core_partner, y_partner, *[at_quarter(ahead[e]) for e in range(1, QUARTERS)]):
        pl.semaphore_signal(barrier, inc=1, device_id=(other, rho), device_id_type=MESH)
    for peer in peers:
        pl.semaphore_signal(barrier, inc=1, device_id=(sub, peer), device_id_type=MESH)

    loads = [
        pltpu.make_async_copy(image_hbm, image, load_sem.at[0]),
        pltpu.make_async_copy(stencil_hbm, stencil, load_sem.at[1]),
        pltpu.make_async_copy(trig_hbm, trig, load_sem.at[2]),
    ]
    for load in loads:
        load.start()

    def build(slot, s, half, child):
        row = s * 4 + half * 2 + child
        shift = lax.broadcasted_iota(jnp.int32, (beams, beams), 0) - stencil[row, 0:1, :]
        cos_row = trig[0, pl.ds(row, 1), :]
        sin_row = trig[1, pl.ds(row, 1), :]
        real = jnp.zeros((beams, beams), F32)
        imag = jnp.zeros((beams, beams), F32)
        for t in range(TAPS):
            hit = shift == t
            real = jnp.where(hit, cos_row * weights[s, t], real)
            imag = jnp.where(hit, sin_row * weights[s, t], imag)
        matrix[slot, 0:beams, 0:beams] = real.astype(BF16)
        matrix[slot, 0:beams, beams:width] = imag.astype(BF16)
        matrix[slot, beams:width, 0:beams] = (-imag).astype(BF16)
        matrix[slot, beams:width, beams:width] = real.astype(BF16)

    def copy_to(src, dst, send, recv, target):
        return pltpu.make_async_remote_copy(
            src_ref=src, dst_ref=dst, send_sem=send, recv_sem=recv, device_id=target, device_id_type=MESH
        )

    for load in loads:
        load.wait()
    for j in range(rows // CHUNK):
        for part in range(2):
            block = image[part, :, j * CHUNK : (j + 1) * CHUNK].astype(F32)
            own[j * CHUNK : (j + 1) * CHUNK, part * beams : (part + 1) * beams] = block.T.astype(BF16)
    low_edge = own[0:16, :].astype(F32)
    high_edge = own[rows - 16 : rows, :].astype(F32)
    edge_out[...] = jnp.concatenate([low_edge[0:8], high_edge[8:16]], axis=0).astype(BF16)
    build(0, 0, core_half, core_half)
    build(1, 0, core_half, 1 - core_half)

    pl.semaphore_wait(barrier, 1 + 1 + QUARTERS - 1 + n_rng - 1)

    def core_copy(rim):
        base, size = (rows, 16) if rim else (0, rows)
        return copy_to(
            own.at[pl.ds(base, size)], got.at[pl.ds(base, size)], core_send.at[rim], core_recv.at[rim], (core_partner, rho)
        )

    below, above = lax.rem(rho + n_rng - 1, n_rng), lax.rem(rho + 1, n_rng)

    def edge(side):
        return copy_to(
            edge_out, edge_in.at[side], edge_send.at[side], edge_recv.at[side], (sub, above if side == 0 else below)
        )

    edge(0).start()
    edge(1).start()
    core_copy(0).start()

    row_id = lax.broadcasted_iota(jnp.int32, (16, width), 0)
    one = jnp.float32(1.0)
    spot = rho * QUARTERS + quarter
    low = jnp.where(rho < n_rng - 1, one, 0.0)
    high = jnp.where(rho > 0, one, 0.0)
    mask = jnp.where(row_id < 8, low, high)
    low = jnp.where(spot < n_rng * QUARTERS - 1, one, 0.0)
    high = jnp.where(spot > 0, one, 0.0)
    chunk_mask = jnp.where(row_id < 8, low, high)

    def rotate(value, g_re, g_im):
        value = value.astype(F32)
        real, imag = value[:, :beams], value[:, beams:]
        return jnp.concatenate(
            [(real * g_re - imag * g_im).astype(BF16), (real * g_im + imag * g_re).astype(BF16)], axis=1
        )

    def factors(re, im, power):
        scale = 1.0 / jnp.sqrt(power + EPS)
        return re * scale, -(im * scale)

    def tally(y, sums):
        real, imag = y[:, :beams], y[:, beams:]
        real_next, imag_next = pltpu.roll(real, beams - 1, 1), pltpu.roll(imag, beams - 1, 1)
        size = real.shape[0]
        products = (
            real * real_next + imag * imag_next,
            real * imag_next - imag * real_next,
            (real * real + imag * imag) * (real_next * real_next + imag_next * imag_next),
        )
        return [a + jnp.sum(p.reshape(size // 8, 8, beams), axis=0) for a, p in zip(sums, products)]

    def zeros():
        return [jnp.zeros((8, beams), F32) for _ in range(3)]

    def spread(base, size, mine, theirs, taps_mine, taps_theirs):
        acc0[pl.ds(base + 8, size), :] = taps_mine[0] * mine + taps_theirs[0] * theirs
        acc1[pl.ds(base, size), :] = taps_mine[1] * mine + taps_theirs[1] * theirs
        acc2[pl.ds(base, size), :] = taps_mine[2] * mine + taps_theirs[2] * theirs

    def close(length):
        acc0[0:8, :] = acc0[length : length + 8, :]
        acc2[length : length + 8, :] = acc2[0:8, :]

    def merge(base, size):
        lower = acc0[base : base + size + 8, :][7 : 7 + size]
        upper = acc2[base : base + size + 8, :][1 : 1 + size]
        return (acc1[base : base + size, :] + lower + upper).astype(BF16)

    line = lax.broadcasted_iota(jnp.int32, (8, beams), 0)

    def sums_copy(s, d, slot):
        return copy_to(
            sums_out.at[s], sums_in.at[s, slot], sums_send.at[s, d], sums_recv.at[s, d], (sub, peers[d])
        )

    def send_sums(s, sums):
        packed = jnp.zeros((8, beams), F32)
        for k in range(3):
            packed = jnp.where(line == k, jnp.sum(sums[k], axis=0, keepdims=True), packed)
        sums_out[s] = packed
        sums_in[s, rho] = packed
        for d in range(n_rng - 1):
            sums_copy(s, d, rho).start()

    def take_sums(s):
        for d in range(n_rng - 1):
            sums_copy(s, d, peers[n_rng - 2 - d]).wait_recv()
        full = sums_in[s, 0]
        for other in range(1, n_rng):
            full = full + sums_in[s, other]
        return factors(full[0:1], full[1:2], full[2:3])

    half_rows = rows // 2

    @pl.loop(0, 2)
    def _(i):
        base = pl.multiple_of(i * half_rows, 16)
        prod[pl.ds(base, half_rows), :] = jnp.dot(
            own[pl.ds(base, half_rows), :], matrix[0], preferred_element_type=F32
        )

    core_mine = [taps[k, core_half, 0] for k in range(3)]
    core_theirs = [taps[k, 1 - core_half, 0] for k in range(3)]
    core_copy(0).wait_recv()

    @pl.loop(0, 2)
    def _(i):
        base = pl.multiple_of(i * half_rows, 16)
        theirs = jnp.dot(got[pl.ds(base, half_rows), :], matrix[1], preferred_element_type=F32)
        spread(base, half_rows, prod[pl.ds(base, half_rows), :], theirs, core_mine, core_theirs)

    edge(0).wait()
    edge(1).wait()
    halo = jnp.concatenate([edge_in[1].astype(F32)[0:8], edge_in[0].astype(F32)[8:16]], axis=0)
    own[rows:total, :] = (halo * mask).astype(BF16)
    core_copy(1).start()
    mine = jnp.dot(own[rows:total, :], matrix[0], preferred_element_type=F32)
    core_copy(1).wait_recv()
    theirs = jnp.dot(got[rows:total, :], matrix[1], preferred_element_type=F32)
    spread(rows, 16, mine, theirs, core_mine, core_theirs)
    close(total)
    sums = zeros()
    for j in range(QUARTERS):
        y = merge(j * CHUNK, CHUNK)
        split_out[j, 0:CHUNK, :] = y
        y = y.astype(F32)
        sums = tally(y, sums)
        prod[j * CHUNK : j * CHUNK + 8, :] = y[0:8]
        prod[(j + 1) * CHUNK - 8 : (j + 1) * CHUNK, :] = y[CHUNK - 8 : CHUNK]
    send_sums(0, sums)
    prod[rows:total, :] = merge(rows, 16).astype(F32) * mask
    for j in range(QUARTERS):
        after = (j + 1) * CHUNK
        before = (j * CHUNK - 8) % total
        split_out[j, CHUNK:WITH_RIM, :] = jnp.concatenate(
            [prod[after : after + 8, :], prod[before : before + 8, :]], axis=0
        ).astype(BF16)

    def split(e, slot):
        return copy_to(
            split_out.at[ahead[e]],
            split_in.at[slot],
            split_send.at[e - 1],
            split_recv.at[e - 1],
            (at_quarter(ahead[e]), rho),
        )

    def fac(e, slot):
        return copy_to(
            fac_out, fac_in.at[slot], fac_send.at[e - 1], fac_recv.at[e - 1], (at_quarter(ahead[e]), rho)
        )

    split(2, quarter).start()
    split_in[quarter] = split_out[quarter]
    g_re, g_im = take_sums(0)
    packed = jnp.where(line == 0, g_re, jnp.where(line == 1, g_im, 0.0))
    fac_out[...] = packed
    fac_in[quarter] = packed
    for e in (1, 3, 2):
        fac(e, quarter).start()
    split(1, quarter).start()
    split(3, quarter).start()

    for half in range(2):
        for child in range(2):
            build(2 + half * 2 + child, 1, half, child)
            build(6 + half * 2 + child, 2, half, child)
    build(10, 3, y_half, y_half)
    build(11, 3, y_half, 1 - y_half)

    def wide_copy(t, d, slot):
        return copy_to(
            wide_out.at[t], wide_in.at[t, slot], wide_send.at[t, d], wide_recv.at[t, d], (sub, peers[d])
        )

    def part_copy(t, e, slot):
        return copy_to(
            part_out.at[t],
            part_in.at[t, slot],
            part_send.at[t, e - 1],
            part_recv.at[t, e - 1],
            (at_quarter(ahead[e]), rho),
        )

    tall = lax.broadcasted_iota(jnp.int32, (16, beams), 0)

    def cross(t, target):
        s = t + 1
        packed = jnp.zeros((16, beams), F32)
        for half in range(2):
            for child in range(2):
                terms[child] = jnp.dot(
                    stacked[child], matrix[2 + 4 * t + half * 2 + child], preferred_element_type=F32
                )
            for pair in range(2):
                block = 2 * pair + half if t == 0 else 2 * half + pair
                at = pair * WITH_RIM
                spread(
                    0,
                    WITH_RIM,
                    terms[0, at : at + WITH_RIM, :],
                    terms[1, at : at + WITH_RIM, :],
                    [taps[k, 0, s] for k in range(3)],
                    [taps[k, 1, s] for k in range(3)],
                )
                close(WITH_RIM)
                y = merge(0, CHUNK)
                target[block, 0:CHUNK, :] = y
                sums = tally(y.astype(F32), zeros())
                target[block, CHUNK:WITH_RIM, :] = (merge(CHUNK, 16).astype(F32) * chunk_mask).astype(BF16)
                for k in range(3):
                    packed = jnp.where(
                        tall == k * 4 + block, jnp.sum(sums[k], axis=0, keepdims=True), packed
                    )
        wide_out[t] = packed
        wide_in[t, rho] = packed
        for d in range(n_rng - 1):
            wide_copy(t, d, rho).start()

    def narrow(t):
        for d in range(n_rng - 1):
            wide_copy(t, d, peers[n_rng - 2 - d]).wait_recv()
        full = wide_in[t, 0]
        for other in range(1, n_rng):
            full = full + wide_in[t, other]
        part_out[t] = full
        part_in[t, quarter] = full
        for e in (2, 1, 3):
            part_copy(t, e, quarter).start()

    def finish(t):
        for e in (1, 3, 2):
            part_copy(t, e, behind[e]).wait_recv()
        full = part_in[t, 0]
        for other in range(1, QUARTERS):
            full = full + part_in[t, other]
        return factors(full[0:4], full[4:8], full[8:12])

    for e in (2, 1, 3):
        fac(e, behind[e]).wait_recv()
        split(e, behind[e]).wait_recv()
    for block in range(QUARTERS):
        stacked[block % 2, (block // 2) * WITH_RIM : (block // 2 + 1) * WITH_RIM, :] = rotate(
            split_in[block], fac_in[block, 0:1, :], fac_in[block, 1:2, :]
        )
    cross(0, middle_y)
    narrow(0)
    g_re, g_im = finish(0)

    for block in range(QUARTERS):
        stacked[block // 2, (block % 2) * WITH_RIM : (block % 2 + 1) * WITH_RIM, :] = rotate(
            middle_y[block], g_re[block : block + 1], g_im[block : block + 1]
        )
    cross(1, back_out)

    def back(e, slot):
        return copy_to(
            back_out.at[ahead[e]],
            back_in.at[slot],
            back_send.at[e - 1],
            back_recv.at[e - 1],
            (at_quarter(ahead[e]), rho),
        )

    def far(e):
        return copy_to(
            back_in.at[behind[e]], far_in.at[behind[e]], far_send.at[e], far_recv.at[e], (y_partner, rho)
        )

    back_in[quarter] = back_out[quarter]
    back(2, quarter).start()
    far(0).start()
    narrow(1)
    back(1, quarter).start()
    back(3, quarter).start()
    back(2, behind[2]).wait_recv()
    far(2).start()
    g_re, g_im = finish(1)
    mine_row = lax.broadcasted_iota(jnp.int32, (4, beams), 0) == quarter
    g_re = jnp.sum(jnp.where(mine_row, g_re, 0.0), axis=0, keepdims=True)
    g_im = jnp.sum(jnp.where(mine_row, g_im, 0.0), axis=0, keepdims=True)
    far_fac_out[...] = jnp.where(line == 0, g_re, jnp.where(line == 1, g_im, 0.0))
    far_fac = copy_to(far_fac_out, far_fac_in, far_send.at[4], far_recv.at[4], (y_partner, rho))
    far_fac.start()
    for e in (1, 3):
        back(e, behind[e]).wait_recv()
        far(e).start()

    core_copy(0).wait_send()
    core_copy(1).wait_send()

    def lay(source, target, re, im):
        for j in range(QUARTERS):
            target[j * CHUNK : (j + 1) * CHUNK, :] = rotate(source[j, 0:CHUNK, :], re, im)
        rim = jnp.concatenate(
            [
                source[QUARTERS - 1, CHUNK:WITH_RIM, :].astype(F32)[0:8],
                source[0, CHUNK:WITH_RIM, :].astype(F32)[8:16],
            ],
            axis=0,
        )
        target[rows:total, :] = rotate(rim, re, im)

    big = total // 3
    lay(back_in, own, g_re, g_im)

    @pl.loop(0, 3)
    def _(i):
        base = pl.multiple_of(i * big, 16)
        prod[pl.ds(base, big), :] = jnp.dot(own[pl.ds(base, big), :], matrix[10], preferred_element_type=F32)

    far_fac.wait_recv()
    for e in range(QUARTERS):
        copy_to(
            back_in.at[behind[e]], far_in.at[behind[e]], far_send.at[e], far_recv.at[e], (y_partner, rho)
        ).wait_recv()
    lay(far_in, got, far_fac_in[0:1, :], far_fac_in[1:2, :])
    y_mine = [taps[k, y_half, 3] for k in range(3)]
    y_theirs = [taps[k, 1 - y_half, 3] for k in range(3)]

    @pl.loop(0, 3)
    def _(i):
        base = pl.multiple_of(i * big, 16)
        theirs = jnp.dot(got[pl.ds(base, big), :], matrix[11], preferred_element_type=F32)
        spread(base, big, prod[pl.ds(base, big), :], theirs, y_mine, y_theirs)

    close(total)
    sums = zeros()
    for j in range(QUARTERS):
        y = merge(j * CHUNK, CHUNK)
        own[j * CHUNK : (j + 1) * CHUNK, :] = y
        sums = tally(y.astype(F32), sums)
    send_sums(1, sums)
    for j in range(QUARTERS):
        y = own[j * CHUNK : (j + 1) * CHUNK, :].astype(F32)
        for part in range(2):
            merged[part, :, j * CHUNK : (j + 1) * CHUNK] = y[:, part * beams : (part + 1) * beams].T.astype(
                BF16
            )
    g_re, g_im = take_sums(1)
    phase[0:1, :] = g_re
    phase[1:2, :] = g_im

    for s in range(2):
        for d in range(n_rng - 1):
            sums_copy(s, d, rho).wait_send()
            wide_copy(s, d, rho).wait_send()
        for e in range(1, QUARTERS):
            part_copy(s, e, quarter).wait_send()
    for e in range(1, QUARTERS):
        split(e, quarter).wait_send()
        fac(e, quarter).wait_send()
        back(e, quarter).wait_send()
    for e in range(QUARTERS):
        far(e).wait_send()
    far_fac.wait_send()


def solution(mesh):
    n_rng = mesh.shape["rng"]

    def on_device(image, stencil, interp_weights, range_taps):
        _, beams, rows = image.shape
        total = rows + 16
        cosines, sines = angle_tables(beams)
        hbm = pl.BlockSpec(memory_space=pltpu.HBM)
        vmem = pl.BlockSpec(memory_space=pltpu.VMEM)
        smem = pl.BlockSpec(memory_space=pltpu.SMEM)
        dma = pltpu.SemaphoreType.DMA
        return pl.pallas_call(
            functools.partial(kernel, n_rng),
            out_shape=(
                jax.ShapeDtypeStruct((2, beams, rows), BF16),
                jax.ShapeDtypeStruct((2, beams), F32),
            ),
            in_specs=[smem, smem, hbm, hbm, hbm],
            out_specs=(vmem, vmem),
            scratch_shapes=[
                pltpu.VMEM((2, beams, rows), BF16),
                pltpu.VMEM((SECTIONS * 4, TAPS, beams), jnp.int32),
                pltpu.VMEM((2, SECTIONS * 4, beams), F32),
                pltpu.VMEM((total, 2 * beams), BF16),
                pltpu.VMEM((total, 2 * beams), BF16),
                pltpu.VMEM((12, 2 * beams, 2 * beams), BF16),
                pltpu.VMEM((total + 8, 2 * beams), F32),
                pltpu.VMEM((total, 2 * beams), F32),
                pltpu.VMEM((total + 8, 2 * beams), F32),
                pltpu.VMEM((total, 2 * beams), F32),
                pltpu.VMEM((16, 2 * beams), BF16),
                pltpu.VMEM((2, 16, 2 * beams), BF16),
                pltpu.VMEM((2, 8, beams), F32),
                pltpu.VMEM((2, n_rng, 8, beams), F32),
                pltpu.VMEM((QUARTERS, WITH_RIM, 2 * beams), BF16),
                pltpu.VMEM((QUARTERS, WITH_RIM, 2 * beams), BF16),
                pltpu.VMEM((2, 2 * WITH_RIM, 2 * beams), BF16),
                pltpu.VMEM((2, 2 * WITH_RIM, 2 * beams), F32),
                pltpu.VMEM((QUARTERS, WITH_RIM, 2 * beams), BF16),
                pltpu.VMEM((QUARTERS, WITH_RIM, 2 * beams), BF16),
                pltpu.VMEM((QUARTERS, WITH_RIM, 2 * beams), BF16),
                pltpu.VMEM((QUARTERS, WITH_RIM, 2 * beams), BF16),
                pltpu.VMEM((8, beams), F32),
                pltpu.VMEM((QUARTERS, 8, beams), F32),
                pltpu.VMEM((8, beams), F32),
                pltpu.VMEM((8, beams), F32),
                pltpu.VMEM((2, 16, beams), F32),
                pltpu.VMEM((2, n_rng, 16, beams), F32),
                pltpu.VMEM((2, 16, beams), F32),
                pltpu.VMEM((2, QUARTERS, 16, beams), F32),
                dma((3,)),
                dma((2,)),
                dma((2,)),
                dma((2,)),
                dma((2,)),
                dma((2, n_rng - 1)),
                dma((2, n_rng - 1)),
                dma((QUARTERS - 1,)),
                dma((QUARTERS - 1,)),
                dma((QUARTERS - 1,)),
                dma((QUARTERS - 1,)),
                dma((QUARTERS + 1,)),
                dma((QUARTERS + 1,)),
                dma((QUARTERS - 1,)),
                dma((QUARTERS - 1,)),
                dma((2, n_rng - 1)),
                dma((2, n_rng - 1)),
                dma((2, QUARTERS - 1)),
                dma((2, QUARTERS - 1)),
            ],
            compiler_params=pltpu.CompilerParams(
                collective_id=0, has_side_effects=True, vmem_limit_bytes=67043328
            ),
        )(
            interp_weights,
            range_taps.transpose(2, 1, 0),
            image,
            stencil.transpose(0, 1, 2, 4, 3).reshape(SECTIONS * 4, TAPS, beams),
            jnp.asarray(np.stack([cosines, sines])),
        )

    return jax.shard_map(
        on_device,
        mesh=mesh,
        in_specs=(P(None, "sub", "rng"), P(), P(), P()),
        out_specs=(P(None, "sub", "rng"), P(None, "sub")),
        check_vma=False,
    )
```

```python
import functools

import jax
import jax.numpy as jnp
import numpy as np
from jax import lax
from jax.experimental import pallas as pl
from jax.experimental.pallas import tpu as pltpu
from jax.sharding import PartitionSpec as P

SECTIONS = 4
TAPS = 4
EPS = 1e-6
QUARTERS = 4
CHUNK = 128
WITH_RIM = CHUNK + 16
PARTS = ((0, CHUNK // 2), (CHUNK // 2, CHUNK // 2), (CHUNK, 16))
RIM = 2
MESH = pl.DeviceIdType.MESH
F32 = jnp.float32
BF16 = jnp.bfloat16


def angle_tables(beams):
    rows = []
    for s in range(SECTIONS):
        for h in range(2):
            for c in range(2):
                pos = np.float32(h * beams) + np.arange(beams, dtype=np.float32) + np.float32(0.5)
                rows.append(np.float32(2 * c - 1) * pos * np.float32(0.37 + 0.11 * s))
    psi = np.stack(rows).astype(np.float64)
    return np.cos(psi).astype(np.float32), np.sin(psi).astype(np.float32)


def kernel(
    n_rng,
    weights,
    taps,
    image_hbm,
    stencil_hbm,
    trig_hbm,
    merged,
    phase,
    image,
    stencil,
    trig,
    own,
    got,
    matrix,
    acc0,
    acc1,
    acc2,
    prod,
    edge_out,
    edge_in,
    sums_out,
    sums_in,
    split_out,
    split_in,
    stacked,
    terms,
    middle_y,
    back_out,
    back_in,
    far_in,
    fac_out,
    fac_in,
    far_fac_out,
    far_fac_in,
    wide_out,
    wide_in,
    part_out,
    part_in,
    load_sem,
    core_send,
    core_recv,
    edge_send,
    edge_recv,
    sums_send,
    sums_recv,
    split_send,
    split_recv,
    back_send,
    back_recv,
    far_send,
    far_recv,
    fac_send,
    fac_recv,
    wide_send,
    wide_recv,
    part_send,
    part_recv,
):
    sub = lax.axis_index("sub")
    rho = lax.axis_index("rng")
    beams = image.shape[1]
    rows = image.shape[2]
    total = rows + 16
    width = 2 * beams
    quarter = lax.rem(sub // 2, QUARTERS)
    core_half = lax.rem(sub, 2)
    y_half = lax.rem(sub // 8, 2)
    core_partner = sub + 1 - 2 * core_half
    y_partner = sub + 8 * (1 - 2 * y_half)
    ahead = [lax.rem(quarter + e, QUARTERS) for e in range(QUARTERS)]
    behind = [lax.rem(quarter + QUARTERS - e, QUARTERS) for e in range(QUARTERS)]
    peers = [lax.rem(rho + d, n_rng) for d in range(1, n_rng)]

    def at_quarter(other):
        return sub + 2 * (other - quarter)

    barrier = pltpu.get_barrier_semaphore()
    for other in (core_partner, y_partner, *[at_quarter(ahead[e]) for e in range(1, QUARTERS)]):
        pl.semaphore_signal(barrier, inc=1, device_id=(other, rho), device_id_type=MESH)
    for peer in peers:
        pl.semaphore_signal(barrier, inc=1, device_id=(sub, peer), device_id_type=MESH)

    loads = [
        pltpu.make_async_copy(image_hbm, image, load_sem.at[0]),
        pltpu.make_async_copy(stencil_hbm, stencil, load_sem.at[1]),
        pltpu.make_async_copy(trig_hbm, trig, load_sem.at[2]),
    ]
    for load in loads:
        load.start()

    def build(slot, s, half, child):
        row = s * 4 + half * 2 + child
        shift = lax.broadcasted_iota(jnp.int32, (beams, beams), 0) - stencil[row, 0:1, :]
        cos_row = trig[0, pl.ds(row, 1), :]
        sin_row = trig[1, pl.ds(row, 1), :]
        real = jnp.zeros((beams, beams), F32)
        imag = jnp.zeros((beams, beams), F32)
        for t in range(TAPS):
            hit = shift == t
            real = jnp.where(hit, cos_row * weights[s, t], real)
            imag = jnp.where(hit, sin_row * weights[s, t], imag)
        matrix[slot, 0:beams, 0:beams] = real.astype(BF16)
        matrix[slot, 0:beams, beams:width] = imag.astype(BF16)
        matrix[slot, beams:width, 0:beams] = (-imag).astype(BF16)
        matrix[slot, beams:width, beams:width] = real.astype(BF16)

    def copy_to(src, dst, send, recv, target):
        return pltpu.make_async_remote_copy(
            src_ref=src, dst_ref=dst, send_sem=send, recv_sem=recv, device_id=target, device_id_type=MESH
        )

    for load in loads:
        load.wait()
    for j in range(rows // CHUNK):
        for part in range(2):
            block = image[part, :, j * CHUNK : (j + 1) * CHUNK].astype(F32)
            own[j * CHUNK : (j + 1) * CHUNK, part * beams : (part + 1) * beams] = block.T.astype(BF16)
    low_edge = own[0:16, :].astype(F32)
    high_edge = own[rows - 16 : rows, :].astype(F32)
    edge_out[...] = jnp.concatenate([low_edge[0:8], high_edge[8:16]], axis=0).astype(BF16)
    build(0, 0, core_half, core_half)
    build(1, 0, core_half, 1 - core_half)

    pl.semaphore_wait(barrier, 1 + 1 + QUARTERS - 1 + n_rng - 1)

    def core_copy(rim):
        base, size = (rows, 16) if rim else (0, rows)
        return copy_to(
            own.at[pl.ds(base, size)], got.at[pl.ds(base, size)], core_send.at[rim], core_recv.at[rim], (core_partner, rho)
        )

    below, above = lax.rem(rho + n_rng - 1, n_rng), lax.rem(rho + 1, n_rng)

    def edge(side):
        return copy_to(
            edge_out, edge_in.at[side], edge_send.at[side], edge_recv.at[side], (sub, above if side == 0 else below)
        )

    edge(0).start()
    edge(1).start()
    core_copy(0).start()

    row_id = lax.broadcasted_iota(jnp.int32, (16, width), 0)
    one = jnp.float32(1.0)
    spot = rho * QUARTERS + quarter
    low = jnp.where(rho < n_rng - 1, one, 0.0)
    high = jnp.where(rho > 0, one, 0.0)
    mask = jnp.where(row_id < 8, low, high)
    low = jnp.where(spot < n_rng * QUARTERS - 1, one, 0.0)
    high = jnp.where(spot > 0, one, 0.0)
    chunk_mask = jnp.where(row_id < 8, low, high)

    def rotate(value, g_re, g_im):
        value = value.astype(F32)
        real, imag = value[:, :beams], value[:, beams:]
        return jnp.concatenate(
            [(real * g_re - imag * g_im).astype(BF16), (real * g_im + imag * g_re).astype(BF16)], axis=1
        )

    def factors(re, im, power):
        scale = 1.0 / jnp.sqrt(power + EPS)
        return re * scale, -(im * scale)

    def tally(y, sums):
        real, imag = y[:, :beams], y[:, beams:]
        real_next, imag_next = pltpu.roll(real, beams - 1, 1), pltpu.roll(imag, beams - 1, 1)
        size = real.shape[0]
        products = (
            real * real_next + imag * imag_next,
            real * imag_next - imag * real_next,
            (real * real + imag * imag) * (real_next * real_next + imag_next * imag_next),
        )
        return [a + jnp.sum(p.reshape(size // 8, 8, beams), axis=0) for a, p in zip(sums, products)]

    def zeros():
        return [jnp.zeros((8, beams), F32) for _ in range(3)]

    def spread(base, size, mine, theirs, taps_mine, taps_theirs):
        acc0[pl.ds(base + 8, size), :] = taps_mine[0] * mine + taps_theirs[0] * theirs
        acc1[pl.ds(base, size), :] = taps_mine[1] * mine + taps_theirs[1] * theirs
        acc2[pl.ds(base, size), :] = taps_mine[2] * mine + taps_theirs[2] * theirs

    def close(length):
        acc0[0:8, :] = acc0[length : length + 8, :]
        acc2[length : length + 8, :] = acc2[0:8, :]

    def merge(base, size):
        lower = acc0[base : base + size + 8, :][7 : 7 + size]
        upper = acc2[base : base + size + 8, :][1 : 1 + size]
        return (acc1[base : base + size, :] + lower + upper).astype(BF16)

    line = lax.broadcasted_iota(jnp.int32, (8, beams), 0)

    def sums_copy(s, d, slot):
        return copy_to(
            sums_out.at[s], sums_in.at[s, slot], sums_send.at[s, d], sums_recv.at[s, d], (sub, peers[d])
        )

    def send_sums(s, sums):
        packed = jnp.zeros((8, beams), F32)
        for k in range(3):
            packed = jnp.where(line == k, jnp.sum(sums[k], axis=0, keepdims=True), packed)
        sums_out[s] = packed
        sums_in[s, rho] = packed
        for d in range(n_rng - 1):
            sums_copy(s, d, rho).start()

    def take_sums(s):
        for d in range(n_rng - 1):
            sums_copy(s, d, peers[n_rng - 2 - d]).wait_recv()
        full = sums_in[s, 0]
        for other in range(1, n_rng):
            full = full + sums_in[s, other]
        return factors(full[0:1], full[1:2], full[2:3])

    half_rows = rows // 2

    @pl.loop(0, 2)
    def _(i):
        base = pl.multiple_of(i * half_rows, 16)
        prod[pl.ds(base, half_rows), :] = jnp.dot(
            own[pl.ds(base, half_rows), :], matrix[0], preferred_element_type=F32
        )

    core_mine = [taps[k, core_half, 0] for k in range(3)]
    core_theirs = [taps[k, 1 - core_half, 0] for k in range(3)]
    core_copy(0).wait_recv()

    @pl.loop(0, 2)
    def _(i):
        base = pl.multiple_of(i * half_rows, 16)
        theirs = jnp.dot(got[pl.ds(base, half_rows), :], matrix[1], preferred_element_type=F32)
        spread(base, half_rows, prod[pl.ds(base, half_rows), :], theirs, core_mine, core_theirs)

    edge(0).wait()
    edge(1).wait()
    halo = jnp.concatenate([edge_in[1].astype(F32)[0:8], edge_in[0].astype(F32)[8:16]], axis=0)
    own[rows:total, :] = (halo * mask).astype(BF16)
    core_copy(1).start()
    mine = jnp.dot(own[rows:total, :], matrix[0], preferred_element_type=F32)
    core_copy(1).wait_recv()
    theirs = jnp.dot(got[rows:total, :], matrix[1], preferred_element_type=F32)
    spread(rows, 16, mine, theirs, core_mine, core_theirs)
    close(total)
    sums = zeros()
    for j in range(QUARTERS):
        y = merge(j * CHUNK, CHUNK)
        split_out[j, 0:CHUNK, :] = y
        y = y.astype(F32)
        sums = tally(y, sums)
        prod[j * CHUNK : j * CHUNK + 8, :] = y[0:8]
        prod[(j + 1) * CHUNK - 8 : (j + 1) * CHUNK, :] = y[CHUNK - 8 : CHUNK]
    send_sums(0, sums)
    prod[rows:total, :] = merge(rows, 16).astype(F32) * mask
    for j in range(QUARTERS):
        after = (j + 1) * CHUNK
        before = (j * CHUNK - 8) % total
        split_out[j, CHUNK:WITH_RIM, :] = jnp.concatenate(
            [prod[after : after + 8, :], prod[before : before + 8, :]], axis=0
        ).astype(BF16)

    def split(e, slot):
        return copy_to(
            split_out.at[ahead[e]],
            split_in.at[slot],
            split_send.at[e - 1],
            split_recv.at[e - 1],
            (at_quarter(ahead[e]), rho),
        )

    def fac(e, slot):
        return copy_to(
            fac_out, fac_in.at[slot], fac_send.at[e - 1], fac_recv.at[e - 1], (at_quarter(ahead[e]), rho)
        )

    split(2, quarter).start()
    split_in[quarter] = split_out[quarter]
    g_re, g_im = take_sums(0)
    packed = jnp.where(line == 0, g_re, jnp.where(line == 1, g_im, 0.0))
    fac_out[...] = packed
    fac_in[quarter] = packed
    for e in (1, 3, 2):
        fac(e, quarter).start()
    split(1, quarter).start()
    split(3, quarter).start()

    for half in range(2):
        for child in range(2):
            build(2 + half * 2 + child, 1, half, child)
            build(6 + half * 2 + child, 2, half, child)
    build(10, 3, y_half, y_half)
    build(11, 3, y_half, 1 - y_half)

    def wide_copy(t, d, slot):
        return copy_to(
            wide_out.at[t], wide_in.at[t, slot], wide_send.at[t, d], wide_recv.at[t, d], (sub, peers[d])
        )

    def part_copy(t, e, slot):
        return copy_to(
            part_out.at[t],
            part_in.at[t, slot],
            part_send.at[t, e - 1],
            part_recv.at[t, e - 1],
            (at_quarter(ahead[e]), rho),
        )

    tall = lax.broadcasted_iota(jnp.int32, (16, beams), 0)

    def cross(t, target):
        s = t + 1
        packed = jnp.zeros((16, beams), F32)
        for half in range(2):
            for child in range(2):
                terms[child] = jnp.dot(
                    stacked[child], matrix[2 + 4 * t + half * 2 + child], preferred_element_type=F32
                )
            for pair in range(2):
                block = 2 * pair + half if t == 0 else 2 * half + pair
                at = pair * WITH_RIM
                spread(
                    0,
                    WITH_RIM,
                    terms[0, at : at + WITH_RIM, :],
                    terms[1, at : at + WITH_RIM, :],
                    [taps[k, 0, s] for k in range(3)],
                    [taps[k, 1, s] for k in range(3)],
                )
                close(WITH_RIM)
                y = merge(0, CHUNK)
                target[block, 0:CHUNK, :] = y
                sums = tally(y.astype(F32), zeros())
                target[block, CHUNK:WITH_RIM, :] = (merge(CHUNK, 16).astype(F32) * chunk_mask).astype(BF16)
                for k in range(3):
                    packed = jnp.where(
                        tall == k * 4 + block, jnp.sum(sums[k], axis=0, keepdims=True), packed
                    )
        wide_out[t] = packed
        wide_in[t, rho] = packed
        for d in range(n_rng - 1):
            wide_copy(t, d, rho).start()

    def narrow(t):
        for d in range(n_rng - 1):
            wide_copy(t, d, peers[n_rng - 2 - d]).wait_recv()
        full = wide_in[t, 0]
        for other in range(1, n_rng):
            full = full + wide_in[t, other]
        part_out[t] = full
        part_in[t, quarter] = full
        for e in (2, 1, 3):
            part_copy(t, e, quarter).start()

    def finish(t):
        for e in (1, 3, 2):
            part_copy(t, e, behind[e]).wait_recv()
        full = part_in[t, 0]
        for other in range(1, QUARTERS):
            full = full + part_in[t, other]
        return factors(full[0:4], full[4:8], full[8:12])

    for e in (0, 2, 1, 3):
        block = behind[e]
        if e > 0:
            fac(e, block).wait_recv()
            split(e, block).wait_recv()
        base = pl.multiple_of(block // 2 * WITH_RIM, 16)
        stacked[lax.rem(block, 2), pl.ds(base, WITH_RIM), :] = rotate(
            split_in[block], fac_in[block, 0:1, :], fac_in[block, 1:2, :]
        )
    cross(0, middle_y)
    narrow(0)
    g_re, g_im = finish(0)

    for block in range(QUARTERS):
        stacked[block // 2, (block % 2) * WITH_RIM : (block % 2 + 1) * WITH_RIM, :] = rotate(
            middle_y[block], g_re[block : block + 1], g_im[block : block + 1]
        )
    cross(1, back_out)

    def ends(slot):
        return lax.rem(slot, QUARTERS - 1) == 0

    def each(slot, action):
        pl.when(ends(slot))(lambda: action(RIM))
        action(0)
        action(1)

    def back(e, slot, k):
        rows_k = pl.ds(*PARTS[k])
        return copy_to(
            back_out.at[ahead[e], rows_k],
            back_in.at[slot, rows_k],
            back_send.at[e - 1, k],
            back_recv.at[e - 1, k],
            (at_quarter(ahead[e]), rho),
        )

    def far(e, k):
        rows_k = pl.ds(*PARTS[k])
        return copy_to(
            back_in.at[behind[e], rows_k],
            far_in.at[behind[e], rows_k],
            far_send.at[e, k],
            far_recv.at[e, k],
            (y_partner, rho),
        )

    def pass_on(e):
        def action(k):
            back(e, behind[e], k).wait_recv()
            far(e, k).start()

        each(behind[e], action)

    back_in[quarter] = back_out[quarter]
    for e in (1, 3):
        each(quarter, lambda k, e=e: back(e, quarter, k).start())
    each(quarter, lambda k: far(0, k).start())
    narrow(1)
    each(quarter, lambda k: back(2, quarter, k).start())
    for e in (1, 3):
        pass_on(e)
    g_re, g_im = finish(1)
    mine_row = lax.broadcasted_iota(jnp.int32, (4, beams), 0) == quarter
    g_re = jnp.sum(jnp.where(mine_row, g_re, 0.0), axis=0, keepdims=True)
    g_im = jnp.sum(jnp.where(mine_row, g_im, 0.0), axis=0, keepdims=True)
    far_fac_out[...] = jnp.where(line == 0, g_re, jnp.where(line == 1, g_im, 0.0))
    far_fac = copy_to(far_fac_out, far_fac_in, far_send.at[4, 0], far_recv.at[4, 0], (y_partner, rho))
    far_fac.start()
    pass_on(2)

    core_copy(0).wait_send()
    core_copy(1).wait_send()

    def rim_of(source, re, im):
        rim = jnp.concatenate(
            [
                source[QUARTERS - 1, CHUNK:WITH_RIM, :].astype(F32)[0:8],
                source[0, CHUNK:WITH_RIM, :].astype(F32)[8:16],
            ],
            axis=0,
        )
        return rotate(rim, re, im)

    for j in range(QUARTERS):
        own[j * CHUNK : (j + 1) * CHUNK, :] = rotate(back_in[j, 0:CHUNK, :], g_re, g_im)
    own[rows:total, :] = rim_of(back_in, g_re, g_im)
    big = total // 3

    @pl.loop(0, 3)
    def _(i):
        base = pl.multiple_of(i * big, 16)
        prod[pl.ds(base, big), :] = jnp.dot(own[pl.ds(base, big), :], matrix[10], preferred_element_type=F32)

    far_fac.wait_recv()
    far_re, far_im = far_fac_in[0:1, :], far_fac_in[1:2, :]
    y_mine = [taps[k, y_half, 3] for k in range(3)]
    y_theirs = [taps[k, 1 - y_half, 3] for k in range(3)]
    for e in (0, 1, 3, 2):
        each(behind[e], lambda k, e=e: far(e, k).wait_recv())
        base = pl.multiple_of(behind[e] * CHUNK, CHUNK)
        theirs = jnp.dot(
            rotate(far_in[behind[e], 0:CHUNK, :], far_re, far_im), matrix[11], preferred_element_type=F32
        )
        spread(base, CHUNK, prod[pl.ds(base, CHUNK), :], theirs, y_mine, y_theirs)
    theirs = jnp.dot(rim_of(far_in, far_re, far_im), matrix[11], preferred_element_type=F32)
    spread(rows, 16, prod[rows:total, :], theirs, y_mine, y_theirs)
    close(total)
    sums = zeros()
    for j in range(QUARTERS):
        y = merge(j * CHUNK, CHUNK)
        own[j * CHUNK : (j + 1) * CHUNK, :] = y
        sums = tally(y.astype(F32), sums)
    send_sums(1, sums)
    for j in range(QUARTERS):
        y = own[j * CHUNK : (j + 1) * CHUNK, :].astype(F32)
        for part in range(2):
            merged[part, :, j * CHUNK : (j + 1) * CHUNK] = y[:, part * beams : (part + 1) * beams].T.astype(
                BF16
            )
    g_re, g_im = take_sums(1)
    phase[0:1, :] = g_re
    phase[1:2, :] = g_im

    for s in range(2):
        for d in range(n_rng - 1):
            sums_copy(s, d, rho).wait_send()
            wide_copy(s, d, rho).wait_send()
        for e in range(1, QUARTERS):
            part_copy(s, e, quarter).wait_send()
    for e in range(1, QUARTERS):
        split(e, quarter).wait_send()
        fac(e, quarter).wait_send()
        each(quarter, lambda k, e=e: back(e, quarter, k).wait_send())
    for e in range(QUARTERS):
        each(behind[e], lambda k, e=e: far(e, k).wait_send())
    far_fac.wait_send()


def solution(mesh):
    n_rng = mesh.shape["rng"]

    def on_device(image, stencil, interp_weights, range_taps):
        _, beams, rows = image.shape
        total = rows + 16
        cosines, sines = angle_tables(beams)
        hbm = pl.BlockSpec(memory_space=pltpu.HBM)
        vmem = pl.BlockSpec(memory_space=pltpu.VMEM)
        smem = pl.BlockSpec(memory_space=pltpu.SMEM)
        dma = pltpu.SemaphoreType.DMA
        return pl.pallas_call(
            functools.partial(kernel, n_rng),
            out_shape=(
                jax.ShapeDtypeStruct((2, beams, rows), BF16),
                jax.ShapeDtypeStruct((2, beams), F32),
            ),
            in_specs=[smem, smem, hbm, hbm, hbm],
            out_specs=(vmem, vmem),
            scratch_shapes=[
                pltpu.VMEM((2, beams, rows), BF16),
                pltpu.VMEM((SECTIONS * 4, TAPS, beams), jnp.int32),
                pltpu.VMEM((2, SECTIONS * 4, beams), F32),
                pltpu.VMEM((total, 2 * beams), BF16),
                pltpu.VMEM((total, 2 * beams), BF16),
                pltpu.VMEM((12, 2 * beams, 2 * beams), BF16),
                pltpu.VMEM((total + 8, 2 * beams), F32),
                pltpu.VMEM((total, 2 * beams), F32),
                pltpu.VMEM((total + 8, 2 * beams), F32),
                pltpu.VMEM((total, 2 * beams), F32),
                pltpu.VMEM((16, 2 * beams), BF16),
                pltpu.VMEM((2, 16, 2 * beams), BF16),
                pltpu.VMEM((2, 8, beams), F32),
                pltpu.VMEM((2, n_rng, 8, beams), F32),
                pltpu.VMEM((QUARTERS, WITH_RIM, 2 * beams), BF16),
                pltpu.VMEM((QUARTERS, WITH_RIM, 2 * beams), BF16),
                pltpu.VMEM((2, 2 * WITH_RIM, 2 * beams), BF16),
                pltpu.VMEM((2, 2 * WITH_RIM, 2 * beams), F32),
                pltpu.VMEM((QUARTERS, WITH_RIM, 2 * beams), BF16),
                pltpu.VMEM((QUARTERS, WITH_RIM, 2 * beams), BF16),
                pltpu.VMEM((QUARTERS, WITH_RIM, 2 * beams), BF16),
                pltpu.VMEM((QUARTERS, WITH_RIM, 2 * beams), BF16),
                pltpu.VMEM((8, beams), F32),
                pltpu.VMEM((QUARTERS, 8, beams), F32),
                pltpu.VMEM((8, beams), F32),
                pltpu.VMEM((8, beams), F32),
                pltpu.VMEM((2, 16, beams), F32),
                pltpu.VMEM((2, n_rng, 16, beams), F32),
                pltpu.VMEM((2, 16, beams), F32),
                pltpu.VMEM((2, QUARTERS, 16, beams), F32),
                dma((3,)),
                dma((2,)),
                dma((2,)),
                dma((2,)),
                dma((2,)),
                dma((2, n_rng - 1)),
                dma((2, n_rng - 1)),
                dma((QUARTERS - 1,)),
                dma((QUARTERS - 1,)),
                dma((QUARTERS - 1, 3)),
                dma((QUARTERS - 1, 3)),
                dma((QUARTERS + 1, 3)),
                dma((QUARTERS + 1, 3)),
                dma((QUARTERS - 1,)),
                dma((QUARTERS - 1,)),
                dma((2, n_rng - 1)),
                dma((2, n_rng - 1)),
                dma((2, QUARTERS - 1)),
                dma((2, QUARTERS - 1)),
            ],
            compiler_params=pltpu.CompilerParams(
                collective_id=0, has_side_effects=True, vmem_limit_bytes=67043328
            ),
        )(
            interp_weights,
            range_taps.transpose(2, 1, 0),
            image,
            stencil.transpose(0, 1, 2, 4, 3).reshape(SECTIONS * 4, TAPS, beams),
            jnp.asarray(np.stack([cosines, sines])),
        )

    return jax.shard_map(
        on_device,
        mesh=mesh,
        in_specs=(P(None, "sub", "rng"), P(), P(), P()),
        out_specs=(P(None, "sub", "rng"), P(None, "sub")),
        check_vma=False,
    )
```

```python
import functools

import jax
import jax.numpy as jnp
import numpy as np
from jax import lax
from jax.experimental import pallas as pl
from jax.experimental.pallas import tpu as pltpu
from jax.sharding import PartitionSpec as P

SECTIONS = 4
TAPS = 4
EPS = 1e-6
QUARTERS = 4
CHUNK = 128
WITH_RIM = CHUNK + 16
PARTS = ((0, CHUNK // 2), (CHUNK // 2, CHUNK // 2), (CHUNK, 16))
RIM = 2
MESH = pl.DeviceIdType.MESH
F32 = jnp.float32
BF16 = jnp.bfloat16


def angle_tables(beams):
    rows = []
    for s in range(SECTIONS):
        for h in range(2):
            for c in range(2):
                pos = np.float32(h * beams) + np.arange(beams, dtype=np.float32) + np.float32(0.5)
                rows.append(np.float32(2 * c - 1) * pos * np.float32(0.37 + 0.11 * s))
    psi = np.stack(rows).astype(np.float64)
    return np.cos(psi).astype(np.float32), np.sin(psi).astype(np.float32)


def kernel(
    n_rng,
    weights,
    taps,
    image_hbm,
    stencil_hbm,
    trig_hbm,
    merged_hbm,
    phase,
    image,
    stencil,
    trig,
    own,
    got,
    matrix,
    acc0,
    acc1,
    acc2,
    prod,
    edge_out,
    edge_in,
    sums_out,
    sums_in,
    split_out,
    split_in,
    stacked,
    terms,
    middle_y,
    back_out,
    back_in,
    far_in,
    fac_out,
    fac_in,
    far_fac_out,
    far_fac_in,
    wide_out,
    wide_in,
    part_out,
    part_in,
    load_sem,
    core_send,
    core_recv,
    edge_send,
    edge_recv,
    sums_send,
    sums_recv,
    split_send,
    split_recv,
    back_send,
    back_recv,
    far_send,
    far_recv,
    fac_send,
    fac_recv,
    wide_send,
    wide_recv,
    part_send,
    part_recv,
):
    sub = lax.axis_index("sub")
    rho = lax.axis_index("rng")
    beams = image.shape[1]
    rows = image.shape[2]
    total = rows + 16
    width = 2 * beams
    quarter = lax.rem(sub // 2, QUARTERS)
    core_half = lax.rem(sub, 2)
    y_half = lax.rem(sub // 8, 2)
    core_partner = sub + 1 - 2 * core_half
    y_partner = sub + 8 * (1 - 2 * y_half)
    ahead = [lax.rem(quarter + e, QUARTERS) for e in range(QUARTERS)]
    behind = [lax.rem(quarter + QUARTERS - e, QUARTERS) for e in range(QUARTERS)]
    peers = [lax.rem(rho + d, n_rng) for d in range(1, n_rng)]

    def at_quarter(other):
        return sub + 2 * (other - quarter)

    barrier = pltpu.get_barrier_semaphore()
    for other in (core_partner, y_partner, *[at_quarter(ahead[e]) for e in range(1, QUARTERS)]):
        pl.semaphore_signal(barrier, inc=1, device_id=(other, rho), device_id_type=MESH)
    for peer in peers:
        pl.semaphore_signal(barrier, inc=1, device_id=(sub, peer), device_id_type=MESH)
    below, above = lax.rem(rho + n_rng - 1, n_rng), lax.rem(rho + 1, n_rng)
    for peer in (below, above):
        pl.semaphore_signal(barrier, inc=1, device_id=(core_partner, peer), device_id_type=MESH)

    loads = [
        pltpu.make_async_copy(image_hbm, image, load_sem.at[0]),
        pltpu.make_async_copy(stencil_hbm, stencil, load_sem.at[1]),
        pltpu.make_async_copy(trig_hbm, trig, load_sem.at[2]),
    ]
    for load in loads:
        load.start()

    def build(slot, s, half, child):
        row = s * 4 + half * 2 + child
        shift = lax.broadcasted_iota(jnp.int32, (beams, beams), 0) - stencil[row, 0:1, :]
        cos_row = trig[0, pl.ds(row, 1), :]
        sin_row = trig[1, pl.ds(row, 1), :]
        real = jnp.zeros((beams, beams), F32)
        imag = jnp.zeros((beams, beams), F32)
        for t in range(TAPS):
            hit = shift == t
            real = jnp.where(hit, cos_row * weights[s, t], real)
            imag = jnp.where(hit, sin_row * weights[s, t], imag)
        matrix[slot, 0:beams, 0:beams] = real.astype(BF16)
        matrix[slot, 0:beams, beams:width] = imag.astype(BF16)
        matrix[slot, beams:width, 0:beams] = (-imag).astype(BF16)
        matrix[slot, beams:width, beams:width] = real.astype(BF16)

    def copy_to(src, dst, send, recv, target):
        return pltpu.make_async_remote_copy(
            src_ref=src, dst_ref=dst, send_sem=send, recv_sem=recv, device_id=target, device_id_type=MESH
        )

    for load in loads:
        load.wait()
    for j in range(rows // CHUNK):
        for part in range(2):
            block = image[part, :, j * CHUNK : (j + 1) * CHUNK].astype(F32)
            own[j * CHUNK : (j + 1) * CHUNK, part * beams : (part + 1) * beams] = block.T.astype(BF16)
    low_edge = own[0:16, :].astype(F32)
    high_edge = own[rows - 16 : rows, :].astype(F32)
    edge_out[...] = jnp.concatenate([low_edge[0:8], high_edge[8:16]], axis=0).astype(BF16)
    build(0, 0, core_half, core_half)
    build(1, 0, core_half, 1 - core_half)

    pl.semaphore_wait(barrier, 1 + 1 + QUARTERS - 1 + n_rng - 1 + 2)

    core_copy = copy_to(
        own.at[pl.ds(0, rows)], got.at[pl.ds(0, rows)], core_send.at[0], core_recv.at[0], (core_partner, rho)
    )

    def edge(whose, side):
        return copy_to(
            edge_out,
            edge_in.at[whose, side],
            edge_send.at[whose, side],
            edge_recv.at[whose, side],
            (core_partner if whose else sub, above if side == 0 else below),
        )

    for whose in range(2):
        for side in range(2):
            edge(whose, side).start()
    core_copy.start()

    row_id = lax.broadcasted_iota(jnp.int32, (16, width), 0)
    one = jnp.float32(1.0)
    spot = rho * QUARTERS + quarter
    low = jnp.where(rho < n_rng - 1, one, 0.0)
    high = jnp.where(rho > 0, one, 0.0)
    mask = jnp.where(row_id < 8, low, high)
    low = jnp.where(spot < n_rng * QUARTERS - 1, one, 0.0)
    high = jnp.where(spot > 0, one, 0.0)
    chunk_mask = jnp.where(row_id < 8, low, high)

    def rotate(value, g_re, g_im):
        value = value.astype(F32)
        real, imag = value[:, :beams], value[:, beams:]
        return jnp.concatenate(
            [(real * g_re - imag * g_im).astype(BF16), (real * g_im + imag * g_re).astype(BF16)], axis=1
        )

    def factors(re, im, power):
        scale = 1.0 / jnp.sqrt(power + EPS)
        return re * scale, -(im * scale)

    def tally(y, sums):
        real, imag = y[:, :beams], y[:, beams:]
        real_next, imag_next = pltpu.roll(real, beams - 1, 1), pltpu.roll(imag, beams - 1, 1)
        size = real.shape[0]
        products = (
            real * real_next + imag * imag_next,
            real * imag_next - imag * real_next,
            (real * real + imag * imag) * (real_next * real_next + imag_next * imag_next),
        )
        return [a + jnp.sum(p.reshape(size // 8, 8, beams), axis=0) for a, p in zip(sums, products)]

    def zeros():
        return [jnp.zeros((8, beams), F32) for _ in range(3)]

    def spread(base, size, mine, theirs, taps_mine, taps_theirs):
        acc0[pl.ds(base + 8, size), :] = taps_mine[0] * mine + taps_theirs[0] * theirs
        acc1[pl.ds(base, size), :] = taps_mine[1] * mine + taps_theirs[1] * theirs
        acc2[pl.ds(base, size), :] = taps_mine[2] * mine + taps_theirs[2] * theirs

    def close(length):
        acc0[0:8, :] = acc0[length : length + 8, :]
        acc2[length : length + 8, :] = acc2[0:8, :]

    def merge(base, size):
        lower = acc0[base : base + size + 8, :][7 : 7 + size]
        upper = acc2[base : base + size + 8, :][1 : 1 + size]
        return (acc1[base : base + size, :] + lower + upper).astype(BF16)

    line = lax.broadcasted_iota(jnp.int32, (8, beams), 0)

    def sums_copy(s, d, slot):
        return copy_to(
            sums_out.at[s], sums_in.at[s, slot], sums_send.at[s, d], sums_recv.at[s, d], (sub, peers[d])
        )

    def send_sums(s, sums):
        packed = jnp.zeros((8, beams), F32)
        for k in range(3):
            packed = jnp.where(line == k, jnp.sum(sums[k], axis=0, keepdims=True), packed)
        sums_out[s] = packed
        sums_in[s, rho] = packed
        for d in range(n_rng - 1):
            sums_copy(s, d, rho).start()

    def take_sums(s):
        for d in range(n_rng - 1):
            sums_copy(s, d, peers[n_rng - 2 - d]).wait_recv()
        full = sums_in[s, 0]
        for other in range(1, n_rng):
            full = full + sums_in[s, other]
        return factors(full[0:1], full[1:2], full[2:3])

    half_rows = rows // 2

    @pl.loop(0, 2)
    def _(i):
        base = pl.multiple_of(i * half_rows, 16)
        prod[pl.ds(base, half_rows), :] = jnp.dot(
            own[pl.ds(base, half_rows), :], matrix[0], preferred_element_type=F32
        )

    core_mine = [taps[k, core_half, 0] for k in range(3)]
    core_theirs = [taps[k, 1 - core_half, 0] for k in range(3)]
    core_copy.wait_recv()

    @pl.loop(0, 2)
    def _(i):
        base = pl.multiple_of(i * half_rows, 16)
        theirs = jnp.dot(got[pl.ds(base, half_rows), :], matrix[1], preferred_element_type=F32)
        spread(base, half_rows, prod[pl.ds(base, half_rows), :], theirs, core_mine, core_theirs)

    sums = zeros()

    def settle(j, sums):
        y = merge(j * CHUNK, CHUNK)
        split_out[j, 0:CHUNK, :] = y
        y = y.astype(F32)
        prod[j * CHUNK : j * CHUNK + 8, :] = y[0:8]
        prod[(j + 1) * CHUNK - 8 : (j + 1) * CHUNK, :] = y[CHUNK - 8 : CHUNK]
        return tally(y, sums)

    for j in range(1, QUARTERS - 1):
        sums = settle(j, sums)
    rims = []
    for whose in range(2):
        edge(whose, 0).wait()
        edge(whose, 1).wait()
        halo = jnp.concatenate(
            [edge_in[whose, 1].astype(F32)[0:8], edge_in[whose, 0].astype(F32)[8:16]], axis=0
        )
        rims.append(
            jnp.dot((halo * mask).astype(BF16), matrix[whose], preferred_element_type=F32)
        )
    spread(rows, 16, rims[0], rims[1], core_mine, core_theirs)
    close(total)
    for j in (0, QUARTERS - 1):
        sums = settle(j, sums)
    send_sums(0, sums)
    prod[rows:total, :] = merge(rows, 16).astype(F32) * mask
    for j in range(QUARTERS):
        after = (j + 1) * CHUNK
        before = (j * CHUNK - 8) % total
        split_out[j, CHUNK:WITH_RIM, :] = jnp.concatenate(
            [prod[after : after + 8, :], prod[before : before + 8, :]], axis=0
        ).astype(BF16)

    def split(e, slot):
        return copy_to(
            split_out.at[ahead[e]],
            split_in.at[slot],
            split_send.at[e - 1],
            split_recv.at[e - 1],
            (at_quarter(ahead[e]), rho),
        )

    def fac(e, slot):
        return copy_to(
            fac_out, fac_in.at[slot], fac_send.at[e - 1], fac_recv.at[e - 1], (at_quarter(ahead[e]), rho)
        )

    split(2, quarter).start()
    split(1, quarter).start()
    split_in[quarter] = split_out[quarter]
    g_re, g_im = take_sums(0)
    packed = jnp.where(line == 0, g_re, jnp.where(line == 1, g_im, 0.0))
    fac_out[...] = packed
    fac_in[quarter] = packed
    for e in (1, 3, 2):
        fac(e, quarter).start()
    split(3, quarter).start()

    for half in range(2):
        for child in range(2):
            build(2 + half * 2 + child, 1, half, child)
            build(6 + half * 2 + child, 2, half, child)
    build(10, 3, y_half, y_half)
    build(11, 3, y_half, 1 - y_half)

    def wide_copy(t, d, slot):
        return copy_to(
            wide_out.at[t], wide_in.at[t, slot], wide_send.at[t, d], wide_recv.at[t, d], (sub, peers[d])
        )

    def part_copy(t, e, slot):
        return copy_to(
            part_out.at[t],
            part_in.at[t, slot],
            part_send.at[t, e - 1],
            part_recv.at[t, e - 1],
            (at_quarter(ahead[e]), rho),
        )

    tall = lax.broadcasted_iota(jnp.int32, (16, beams), 0)

    def cross(t, target):
        s = t + 1
        packed = jnp.zeros((16, beams), F32)
        for half in range(2):
            for child in range(2):
                terms[child] = jnp.dot(
                    stacked[child], matrix[2 + 4 * t + half * 2 + child], preferred_element_type=F32
                )
            for pair in range(2):
                block = 2 * pair + half if t == 0 else 2 * half + pair
                at = pair * WITH_RIM
                spread(
                    0,
                    WITH_RIM,
                    terms[0, at : at + WITH_RIM, :],
                    terms[1, at : at + WITH_RIM, :],
                    [taps[k, 0, s] for k in range(3)],
                    [taps[k, 1, s] for k in range(3)],
                )
                close(WITH_RIM)
                y = merge(0, CHUNK)
                target[block, 0:CHUNK, :] = y
                sums = tally(y.astype(F32), zeros())
                target[block, CHUNK:WITH_RIM, :] = (merge(CHUNK, 16).astype(F32) * chunk_mask).astype(BF16)
                for k in range(3):
                    packed = jnp.where(
                        tall == k * 4 + block, jnp.sum(sums[k], axis=0, keepdims=True), packed
                    )
        wide_out[t] = packed
        wide_in[t, rho] = packed
        for d in range(n_rng - 1):
            wide_copy(t, d, rho).start()

    def narrow(t):
        for d in range(n_rng - 1):
            wide_copy(t, d, peers[n_rng - 2 - d]).wait_recv()
        full = wide_in[t, 0]
        for other in range(1, n_rng):
            full = full + wide_in[t, other]
        part_out[t] = full
        part_in[t, quarter] = full
        for e in (2, 1, 3):
            part_copy(t, e, quarter).start()

    def finish(t):
        for e in (1, 3, 2):
            part_copy(t, e, behind[e]).wait_recv()
        full = part_in[t, 0]
        for other in range(1, QUARTERS):
            full = full + part_in[t, other]
        return factors(full[0:4], full[4:8], full[8:12])

    for e in (0, 2, 1, 3):
        block = behind[e]
        if e > 0:
            fac(e, block).wait_recv()
            split(e, block).wait_recv()
        base = pl.multiple_of(block // 2 * WITH_RIM, 16)
        stacked[lax.rem(block, 2), pl.ds(base, WITH_RIM), :] = rotate(
            split_in[block], fac_in[block, 0:1, :], fac_in[block, 1:2, :]
        )
    cross(0, middle_y)
    narrow(0)
    g_re, g_im = finish(0)

    for block in range(QUARTERS):
        stacked[block // 2, (block % 2) * WITH_RIM : (block % 2 + 1) * WITH_RIM, :] = rotate(
            middle_y[block], g_re[block : block + 1], g_im[block : block + 1]
        )
    cross(1, back_out)

    def ends(slot):
        return lax.rem(slot, QUARTERS - 1) == 0

    def each(slot, action):
        pl.when(ends(slot))(lambda: action(RIM))
        action(0)
        action(1)

    def back(e, slot, k):
        rows_k = pl.ds(*PARTS[k])
        return copy_to(
            back_out.at[ahead[e], rows_k],
            back_in.at[slot, rows_k],
            back_send.at[e - 1, k],
            back_recv.at[e - 1, k],
            (at_quarter(ahead[e]), rho),
        )

    def far(e, k):
        rows_k = pl.ds(*PARTS[k])
        return copy_to(
            back_in.at[behind[e], rows_k],
            far_in.at[behind[e], rows_k],
            far_send.at[e, k],
            far_recv.at[e, k],
            (y_partner, rho),
        )

    def pass_on(e):
        def action(k):
            back(e, behind[e], k).wait_recv()
            far(e, k).start()

        each(behind[e], action)

    back_in[quarter] = back_out[quarter]
    for e in (1, 3):
        each(quarter, lambda k, e=e: back(e, quarter, k).start())
    each(quarter, lambda k: far(0, k).start())
    narrow(1)
    each(quarter, lambda k: back(2, quarter, k).start())
    for e in (1, 3):
        pass_on(e)
    g_re, g_im = finish(1)
    mine_row = lax.broadcasted_iota(jnp.int32, (4, beams), 0) == quarter
    g_re = jnp.sum(jnp.where(mine_row, g_re, 0.0), axis=0, keepdims=True)
    g_im = jnp.sum(jnp.where(mine_row, g_im, 0.0), axis=0, keepdims=True)
    far_fac_out[...] = jnp.where(line == 0, g_re, jnp.where(line == 1, g_im, 0.0))
    far_fac = copy_to(far_fac_out, far_fac_in, far_send.at[4, 0], far_recv.at[4, 0], (y_partner, rho))
    far_fac.start()
    pass_on(2)

    core_copy.wait_send()

    def rim_of(source, re, im):
        rim = jnp.concatenate(
            [
                source[QUARTERS - 1, CHUNK:WITH_RIM, :].astype(F32)[0:8],
                source[0, CHUNK:WITH_RIM, :].astype(F32)[8:16],
            ],
            axis=0,
        )
        return rotate(rim, re, im)

    for j in range(QUARTERS):
        own[j * CHUNK : (j + 1) * CHUNK, :] = rotate(back_in[j, 0:CHUNK, :], g_re, g_im)
    own[rows:total, :] = rim_of(back_in, g_re, g_im)
    big = total // 3

    @pl.loop(0, 3)
    def _(i):
        base = pl.multiple_of(i * big, 16)
        prod[pl.ds(base, big), :] = jnp.dot(own[pl.ds(base, big), :], matrix[10], preferred_element_type=F32)

    far_fac.wait_recv()
    far_re, far_im = far_fac_in[0:1, :], far_fac_in[1:2, :]
    y_mine = [taps[k, y_half, 3] for k in range(3)]
    y_theirs = [taps[k, 1 - y_half, 3] for k in range(3)]
    for e in (0, 1, 3, 2):
        each(behind[e], lambda k, e=e: far(e, k).wait_recv())
        base = pl.multiple_of(behind[e] * CHUNK, CHUNK)
        theirs = jnp.dot(
            rotate(far_in[behind[e], 0:CHUNK, :], far_re, far_im), matrix[11], preferred_element_type=F32
        )
        spread(base, CHUNK, prod[pl.ds(base, CHUNK), :], theirs, y_mine, y_theirs)
    theirs = jnp.dot(rim_of(far_in, far_re, far_im), matrix[11], preferred_element_type=F32)
    spread(rows, 16, prod[rows:total, :], theirs, y_mine, y_theirs)
    close(total)
    sums = zeros()
    for j in range(QUARTERS):
        y = merge(j * CHUNK, CHUNK)
        own[j * CHUNK : (j + 1) * CHUNK, :] = y
        sums = tally(y.astype(F32), sums)
    send_sums(1, sums)
    for j in range(QUARTERS):
        y = own[j * CHUNK : (j + 1) * CHUNK, :].astype(F32)
        for part in range(2):
            image[part, :, j * CHUNK : (j + 1) * CHUNK] = y[:, part * beams : (part + 1) * beams].T.astype(
                BF16
            )
    out = pltpu.make_async_copy(image, merged_hbm, load_sem.at[0])
    out.start()
    g_re, g_im = take_sums(1)
    phase[0:1, :] = g_re
    phase[1:2, :] = g_im

    for s in range(2):
        for d in range(n_rng - 1):
            sums_copy(s, d, rho).wait_send()
            wide_copy(s, d, rho).wait_send()
        for e in range(1, QUARTERS):
            part_copy(s, e, quarter).wait_send()
    for e in range(1, QUARTERS):
        split(e, quarter).wait_send()
        fac(e, quarter).wait_send()
        each(quarter, lambda k, e=e: back(e, quarter, k).wait_send())
    for e in range(QUARTERS):
        each(behind[e], lambda k, e=e: far(e, k).wait_send())
    far_fac.wait_send()
    out.wait()


def solution(mesh):
    n_rng = mesh.shape["rng"]

    def on_device(image, stencil, interp_weights, range_taps):
        _, beams, rows = image.shape
        total = rows + 16
        cosines, sines = angle_tables(beams)
        hbm = pl.BlockSpec(memory_space=pltpu.HBM)
        vmem = pl.BlockSpec(memory_space=pltpu.VMEM)
        smem = pl.BlockSpec(memory_space=pltpu.SMEM)
        dma = pltpu.SemaphoreType.DMA
        return pl.pallas_call(
            functools.partial(kernel, n_rng),
            out_shape=(
                jax.ShapeDtypeStruct((2, beams, rows), BF16),
                jax.ShapeDtypeStruct((2, beams), F32),
            ),
            in_specs=[smem, smem, hbm, hbm, hbm],
            out_specs=(hbm, vmem),
            scratch_shapes=[
                pltpu.VMEM((2, beams, rows), BF16),
                pltpu.VMEM((SECTIONS * 4, TAPS, beams), jnp.int32),
                pltpu.VMEM((2, SECTIONS * 4, beams), F32),
                pltpu.VMEM((total, 2 * beams), BF16),
                pltpu.VMEM((total, 2 * beams), BF16),
                pltpu.VMEM((12, 2 * beams, 2 * beams), BF16),
                pltpu.VMEM((total + 8, 2 * beams), F32),
                pltpu.VMEM((total, 2 * beams), F32),
                pltpu.VMEM((total + 8, 2 * beams), F32),
                pltpu.VMEM((total, 2 * beams), F32),
                pltpu.VMEM((16, 2 * beams), BF16),
                pltpu.VMEM((2, 2, 16, 2 * beams), BF16),
                pltpu.VMEM((2, 8, beams), F32),
                pltpu.VMEM((2, n_rng, 8, beams), F32),
                pltpu.VMEM((QUARTERS, WITH_RIM, 2 * beams), BF16),
                pltpu.VMEM((QUARTERS, WITH_RIM, 2 * beams), BF16),
                pltpu.VMEM((2, 2 * WITH_RIM, 2 * beams), BF16),
                pltpu.VMEM((2, 2 * WITH_RIM, 2 * beams), F32),
                pltpu.VMEM((QUARTERS, WITH_RIM, 2 * beams), BF16),
                pltpu.VMEM((QUARTERS, WITH_RIM, 2 * beams), BF16),
                pltpu.VMEM((QUARTERS, WITH_RIM, 2 * beams), BF16),
                pltpu.VMEM((QUARTERS, WITH_RIM, 2 * beams), BF16),
                pltpu.VMEM((8, beams), F32),
                pltpu.VMEM((QUARTERS, 8, beams), F32),
                pltpu.VMEM((8, beams), F32),
                pltpu.VMEM((8, beams), F32),
                pltpu.VMEM((2, 16, beams), F32),
                pltpu.VMEM((2, n_rng, 16, beams), F32),
                pltpu.VMEM((2, 16, beams), F32),
                pltpu.VMEM((2, QUARTERS, 16, beams), F32),
                dma((3,)),
                dma((1,)),
                dma((1,)),
                dma((2, 2)),
                dma((2, 2)),
                dma((2, n_rng - 1)),
                dma((2, n_rng - 1)),
                dma((QUARTERS - 1,)),
                dma((QUARTERS - 1,)),
                dma((QUARTERS - 1, 3)),
                dma((QUARTERS - 1, 3)),
                dma((QUARTERS + 1, 3)),
                dma((QUARTERS + 1, 3)),
                dma((QUARTERS - 1,)),
                dma((QUARTERS - 1,)),
                dma((2, n_rng - 1)),
                dma((2, n_rng - 1)),
                dma((2, QUARTERS - 1)),
                dma((2, QUARTERS - 1)),
            ],
            compiler_params=pltpu.CompilerParams(
                collective_id=0, has_side_effects=True, vmem_limit_bytes=67043328
            ),
        )(
            interp_weights,
            range_taps.transpose(2, 1, 0),
            image,
            stencil.transpose(0, 1, 2, 4, 3).reshape(SECTIONS * 4, TAPS, beams),
            jnp.asarray(np.stack([cosines, sines])),
        )

    return jax.shard_map(
        on_device,
        mesh=mesh,
        in_specs=(P(None, "sub", "rng"), P(), P(), P()),
        out_specs=(P(None, "sub", "rng"), P(None, "sub")),
        check_vma=False,
    )
```

```python
import functools

import jax
import jax.numpy as jnp
import numpy as np
from jax import lax
from jax.experimental import pallas as pl
from jax.experimental.pallas import tpu as pltpu
from jax.sharding import PartitionSpec as P

SECTIONS = 4
TAPS = 4
EPS = 1e-6
QUARTERS = 4
CHUNK = 128
WITH_RIM = CHUNK + 16
PARTS = ((0, CHUNK // 2), (CHUNK // 2, CHUNK // 2), (CHUNK, 16))
RIM = 2
MESH = pl.DeviceIdType.MESH
F32 = jnp.float32
BF16 = jnp.bfloat16


def angle_tables(beams):
    rows = []
    for s in range(SECTIONS):
        for h in range(2):
            for c in range(2):
                pos = np.float32(h * beams) + np.arange(beams, dtype=np.float32) + np.float32(0.5)
                rows.append(np.float32(2 * c - 1) * pos * np.float32(0.37 + 0.11 * s))
    psi = np.stack(rows).astype(np.float64)
    return np.cos(psi).astype(np.float32), np.sin(psi).astype(np.float32)


def kernel(
    n_rng,
    weights,
    taps,
    image_hbm,
    stencil_hbm,
    trig_hbm,
    merged_hbm,
    phase,
    image,
    stencil,
    trig,
    own,
    got,
    matrix,
    acc0,
    acc1,
    acc2,
    prod,
    edge_out,
    edge_in,
    sums_out,
    sums_in,
    split_out,
    split_in,
    stacked,
    terms,
    middle_y,
    back_out,
    back_in,
    far_in,
    fac_out,
    fac_in,
    far_fac_out,
    far_fac_in,
    wide_out,
    wide_in,
    part_out,
    part_in,
    load_sem,
    core_send,
    core_recv,
    edge_send,
    edge_recv,
    sums_send,
    sums_recv,
    split_send,
    split_recv,
    back_send,
    back_recv,
    far_send,
    far_recv,
    fac_send,
    fac_recv,
    wide_send,
    wide_recv,
    part_send,
    part_recv,
):
    sub = lax.axis_index("sub")
    rho = lax.axis_index("rng")
    beams = image.shape[1]
    rows = image.shape[2]
    total = rows + 16
    width = 2 * beams
    quarter = lax.rem(sub // 2, QUARTERS)
    core_half = lax.rem(sub, 2)
    y_half = lax.rem(sub // 8, 2)
    core_partner = sub + 1 - 2 * core_half
    y_partner = sub + 8 * (1 - 2 * y_half)
    ahead = [lax.rem(quarter + e, QUARTERS) for e in range(QUARTERS)]
    behind = [lax.rem(quarter + QUARTERS - e, QUARTERS) for e in range(QUARTERS)]
    peers = [lax.rem(rho + d, n_rng) for d in range(1, n_rng)]

    def at_quarter(other):
        return sub + 2 * (other - quarter)

    barrier = pltpu.get_barrier_semaphore()
    for other in (core_partner, y_partner, *[at_quarter(ahead[e]) for e in range(1, QUARTERS)]):
        pl.semaphore_signal(barrier, inc=1, device_id=(other, rho), device_id_type=MESH)
    for peer in peers:
        pl.semaphore_signal(barrier, inc=1, device_id=(sub, peer), device_id_type=MESH)
    below, above = lax.rem(rho + n_rng - 1, n_rng), lax.rem(rho + 1, n_rng)
    for peer in (below, above):
        pl.semaphore_signal(barrier, inc=1, device_id=(core_partner, peer), device_id_type=MESH)

    loads = [
        pltpu.make_async_copy(image_hbm, image, load_sem.at[0]),
        pltpu.make_async_copy(stencil_hbm, stencil, load_sem.at[1]),
        pltpu.make_async_copy(trig_hbm, trig, load_sem.at[2]),
    ]
    for load in loads:
        load.start()

    def build(slot, s, half, child):
        row = s * 4 + half * 2 + child
        shift = lax.broadcasted_iota(jnp.int32, (beams, beams), 0) - stencil[row, 0:1, :]
        cos_row = trig[0, pl.ds(row, 1), :]
        sin_row = trig[1, pl.ds(row, 1), :]
        real = jnp.zeros((beams, beams), F32)
        imag = jnp.zeros((beams, beams), F32)
        for t in range(TAPS):
            hit = shift == t
            real = jnp.where(hit, cos_row * weights[s, t], real)
            imag = jnp.where(hit, sin_row * weights[s, t], imag)
        matrix[slot, 0:beams, 0:beams] = real.astype(BF16)
        matrix[slot, 0:beams, beams:width] = imag.astype(BF16)
        matrix[slot, beams:width, 0:beams] = (-imag).astype(BF16)
        matrix[slot, beams:width, beams:width] = real.astype(BF16)

    def copy_to(src, dst, send, recv, target):
        return pltpu.make_async_remote_copy(
            src_ref=src, dst_ref=dst, send_sem=send, recv_sem=recv, device_id=target, device_id_type=MESH
        )

    for load in loads:
        load.wait()
    for j in range(rows // CHUNK):
        for part in range(2):
            block = image[part, :, j * CHUNK : (j + 1) * CHUNK].astype(F32)
            own[j * CHUNK : (j + 1) * CHUNK, part * beams : (part + 1) * beams] = block.T.astype(BF16)
    low_edge = own[0:16, :].astype(F32)
    high_edge = own[rows - 16 : rows, :].astype(F32)
    edge_out[...] = jnp.concatenate([low_edge[0:8], high_edge[8:16]], axis=0).astype(BF16)
    build(0, 0, core_half, core_half)
    build(1, 0, core_half, 1 - core_half)

    pl.semaphore_wait(barrier, 1 + 1 + QUARTERS - 1 + n_rng - 1 + 2)

    core_copy = copy_to(
        own.at[pl.ds(0, rows)], got.at[pl.ds(0, rows)], core_send.at[0], core_recv.at[0], (core_partner, rho)
    )

    def edge(whose, side):
        return copy_to(
            edge_out,
            edge_in.at[whose, side],
            edge_send.at[whose, side],
            edge_recv.at[whose, side],
            (core_partner if whose else sub, above if side == 0 else below),
        )

    for whose in range(2):
        for side in range(2):
            edge(whose, side).start()
    core_copy.start()

    row_id = lax.broadcasted_iota(jnp.int32, (16, width), 0)
    one = jnp.float32(1.0)
    spot = rho * QUARTERS + quarter
    low = jnp.where(rho < n_rng - 1, one, 0.0)
    high = jnp.where(rho > 0, one, 0.0)
    mask = jnp.where(row_id < 8, low, high)
    low = jnp.where(spot < n_rng * QUARTERS - 1, one, 0.0)
    high = jnp.where(spot > 0, one, 0.0)
    chunk_mask = jnp.where(row_id < 8, low, high)

    def rotate(value, g_re, g_im):
        value = value.astype(F32)
        real, imag = value[:, :beams], value[:, beams:]
        return jnp.concatenate(
            [(real * g_re - imag * g_im).astype(BF16), (real * g_im + imag * g_re).astype(BF16)], axis=1
        )

    def factors(re, im, power):
        scale = 1.0 / jnp.sqrt(power + EPS)
        return re * scale, -(im * scale)

    def tally(y, sums):
        real, imag = y[:, :beams], y[:, beams:]
        real_next, imag_next = pltpu.roll(real, beams - 1, 1), pltpu.roll(imag, beams - 1, 1)
        size = real.shape[0]
        products = (
            real * real_next + imag * imag_next,
            real * imag_next - imag * real_next,
            (real * real + imag * imag) * (real_next * real_next + imag_next * imag_next),
        )
        return [a + jnp.sum(p.reshape(size // 8, 8, beams), axis=0) for a, p in zip(sums, products)]

    def zeros():
        return [jnp.zeros((8, beams), F32) for _ in range(3)]

    def spread(base, size, mine, theirs, taps_mine, taps_theirs):
        acc0[pl.ds(base + 8, size), :] = taps_mine[0] * mine + taps_theirs[0] * theirs
        acc1[pl.ds(base, size), :] = taps_mine[1] * mine + taps_theirs[1] * theirs
        acc2[pl.ds(base, size), :] = taps_mine[2] * mine + taps_theirs[2] * theirs

    def close(length):
        acc0[0:8, :] = acc0[length : length + 8, :]
        acc2[length : length + 8, :] = acc2[0:8, :]

    def merge(base, size):
        lower = acc0[base : base + size + 8, :][7 : 7 + size]
        upper = acc2[base : base + size + 8, :][1 : 1 + size]
        return (acc1[base : base + size, :] + lower + upper).astype(BF16)

    line = lax.broadcasted_iota(jnp.int32, (8, beams), 0)

    def sums_copy(s, d, slot):
        return copy_to(
            sums_out.at[s], sums_in.at[s, slot], sums_send.at[s, d], sums_recv.at[s, d], (sub, peers[d])
        )

    def send_sums(s, sums):
        packed = jnp.zeros((8, beams), F32)
        for k in range(3):
            packed = jnp.where(line == k, jnp.sum(sums[k], axis=0, keepdims=True), packed)
        sums_out[s] = packed
        sums_in[s, rho] = packed
        for d in range(n_rng - 1):
            sums_copy(s, d, rho).start()

    def take_sums(s):
        for d in range(n_rng - 1):
            sums_copy(s, d, peers[n_rng - 2 - d]).wait_recv()
        full = sums_in[s, 0]
        for other in range(1, n_rng):
            full = full + sums_in[s, other]
        return factors(full[0:1], full[1:2], full[2:3])

    half_rows = rows // 2

    @pl.loop(0, 2)
    def _(i):
        base = pl.multiple_of(i * half_rows, 16)
        prod[pl.ds(base, half_rows), :] = jnp.dot(
            own[pl.ds(base, half_rows), :], matrix[0], preferred_element_type=F32
        )

    core_mine = [taps[k, core_half, 0] for k in range(3)]
    core_theirs = [taps[k, 1 - core_half, 0] for k in range(3)]
    core_copy.wait_recv()

    @pl.loop(0, 2)
    def _(i):
        base = pl.multiple_of(i * half_rows, 16)
        theirs = jnp.dot(got[pl.ds(base, half_rows), :], matrix[1], preferred_element_type=F32)
        spread(base, half_rows, prod[pl.ds(base, half_rows), :], theirs, core_mine, core_theirs)

    sums = zeros()

    def settle(j, sums):
        y = merge(j * CHUNK, CHUNK)
        split_out[j, 0:CHUNK, :] = y
        y = y.astype(F32)
        prod[j * CHUNK : j * CHUNK + 8, :] = y[0:8]
        prod[(j + 1) * CHUNK - 8 : (j + 1) * CHUNK, :] = y[CHUNK - 8 : CHUNK]
        return tally(y, sums)

    for j in range(1, QUARTERS - 1):
        sums = settle(j, sums)
    rims = []
    for whose in range(2):
        edge(whose, 0).wait()
        edge(whose, 1).wait()
        halo = jnp.concatenate(
            [edge_in[whose, 1].astype(F32)[0:8], edge_in[whose, 0].astype(F32)[8:16]], axis=0
        )
        rims.append(
            jnp.dot((halo * mask).astype(BF16), matrix[whose], preferred_element_type=F32)
        )
    spread(rows, 16, rims[0], rims[1], core_mine, core_theirs)
    close(total)
    for j in (0, QUARTERS - 1):
        sums = settle(j, sums)
    send_sums(0, sums)
    prod[rows:total, :] = merge(rows, 16).astype(F32) * mask
    for j in range(QUARTERS):
        after = (j + 1) * CHUNK
        before = (j * CHUNK - 8) % total
        split_out[j, CHUNK:WITH_RIM, :] = jnp.concatenate(
            [prod[after : after + 8, :], prod[before : before + 8, :]], axis=0
        ).astype(BF16)

    def split(e, slot):
        return copy_to(
            split_out.at[ahead[e]],
            split_in.at[slot],
            split_send.at[e - 1],
            split_recv.at[e - 1],
            (at_quarter(ahead[e]), rho),
        )

    def fac(e, slot):
        return copy_to(
            fac_out, fac_in.at[slot], fac_send.at[e - 1], fac_recv.at[e - 1], (at_quarter(ahead[e]), rho)
        )

    split(2, quarter).start()
    split(1, quarter).start()
    split_in[quarter] = split_out[quarter]
    g_re, g_im = take_sums(0)
    packed = jnp.where(line == 0, g_re, jnp.where(line == 1, g_im, 0.0))
    fac_out[...] = packed
    fac_in[quarter] = packed
    for e in (1, 3, 2):
        fac(e, quarter).start()
    split(3, quarter).start()

    for half in range(2):
        for child in range(2):
            build(2 + half * 2 + child, 1, half, child)
            build(6 + half * 2 + child, 2, half, child)
    build(10, 3, y_half, y_half)
    build(11, 3, y_half, 1 - y_half)

    def wide_copy(t, d, slot):
        return copy_to(
            wide_out.at[t], wide_in.at[t, slot], wide_send.at[t, d], wide_recv.at[t, d], (sub, peers[d])
        )

    def part_copy(t, e, slot):
        return copy_to(
            part_out.at[t],
            part_in.at[t, slot],
            part_send.at[t, e - 1],
            part_recv.at[t, e - 1],
            (at_quarter(ahead[e]), rho),
        )

    lanes = beams // 2
    tall = lax.broadcasted_iota(jnp.int32, (24, lanes), 0)

    def cross(t, target):
        s = t + 1
        packed = jnp.zeros((24, lanes), F32)
        for half in range(2):
            for child in range(2):
                terms[child] = jnp.dot(
                    stacked[child], matrix[2 + 4 * t + half * 2 + child], preferred_element_type=F32
                )
            for pair in range(2):
                block = 2 * pair + half if t == 0 else 2 * half + pair
                at = pair * WITH_RIM
                spread(
                    0,
                    WITH_RIM,
                    terms[0, at : at + WITH_RIM, :],
                    terms[1, at : at + WITH_RIM, :],
                    [taps[k, 0, s] for k in range(3)],
                    [taps[k, 1, s] for k in range(3)],
                )
                close(WITH_RIM)
                y = merge(0, CHUNK)
                target[block, 0:CHUNK, :] = y
                sums = tally(y.astype(F32), zeros())
                target[block, CHUNK:WITH_RIM, :] = (merge(CHUNK, 16).astype(F32) * chunk_mask).astype(BF16)
                for k in range(3):
                    value = jnp.sum(sums[k], axis=0, keepdims=True)
                    for side in range(2):
                        packed = jnp.where(
                            tall == k * 8 + side * 4 + block,
                            value[:, side * lanes : (side + 1) * lanes],
                            packed,
                        )
        wide_out[t] = packed
        wide_in[t, rho] = packed
        for d in range(n_rng - 1):
            wide_copy(t, d, rho).start()

    def narrow(t):
        for d in range(n_rng - 1):
            wide_copy(t, d, peers[n_rng - 2 - d]).wait_recv()
        full = wide_in[t, 0]
        for other in range(1, n_rng):
            full = full + wide_in[t, other]
        part_out[t] = full
        part_in[t, quarter] = full
        for e in (2, 1, 3):
            part_copy(t, e, quarter).start()

    def finish(t):
        for e in (1, 3, 2):
            part_copy(t, e, behind[e]).wait_recv()
        full = part_in[t, 0]
        for other in range(1, QUARTERS):
            full = full + part_in[t, other]
        whole = [jnp.concatenate([full[k : k + 4], full[k + 4 : k + 8]], axis=1) for k in (0, 8, 16)]
        return factors(*whole)

    for e in (0, 2, 1, 3):
        block = behind[e]
        if e > 0:
            fac(e, block).wait_recv()
            split(e, block).wait_recv()
        base = pl.multiple_of(block // 2 * WITH_RIM, 16)
        stacked[lax.rem(block, 2), pl.ds(base, WITH_RIM), :] = rotate(
            split_in[block], fac_in[block, 0:1, :], fac_in[block, 1:2, :]
        )
    cross(0, middle_y)
    narrow(0)
    g_re, g_im = finish(0)

    for block in range(QUARTERS):
        stacked[block // 2, (block % 2) * WITH_RIM : (block % 2 + 1) * WITH_RIM, :] = rotate(
            middle_y[block], g_re[block : block + 1], g_im[block : block + 1]
        )
    cross(1, back_out)

    def ends(slot):
        return lax.rem(slot, QUARTERS - 1) == 0

    def each(slot, action):
        pl.when(ends(slot))(lambda: action(RIM))
        action(0)
        action(1)

    def back(e, slot, k):
        rows_k = pl.ds(*PARTS[k])
        return copy_to(
            back_out.at[ahead[e], rows_k],
            back_in.at[slot, rows_k],
            back_send.at[e - 1, k],
            back_recv.at[e - 1, k],
            (at_quarter(ahead[e]), rho),
        )

    def far(e, k):
        rows_k = pl.ds(*PARTS[k])
        return copy_to(
            back_in.at[behind[e], rows_k],
            far_in.at[behind[e], rows_k],
            far_send.at[e, k],
            far_recv.at[e, k],
            (y_partner, rho),
        )

    def pass_on(e):
        def action(k):
            back(e, behind[e], k).wait_recv()
            far(e, k).start()

        each(behind[e], action)

    back_in[quarter] = back_out[quarter]
    for e in (1, 3):
        each(quarter, lambda k, e=e: back(e, quarter, k).start())
    each(quarter, lambda k: far(0, k).start())
    narrow(1)
    each(quarter, lambda k: back(2, quarter, k).start())
    for e in (1, 3):
        pass_on(e)
    g_re, g_im = finish(1)
    mine_row = lax.broadcasted_iota(jnp.int32, (4, beams), 0) == quarter
    g_re = jnp.sum(jnp.where(mine_row, g_re, 0.0), axis=0, keepdims=True)
    g_im = jnp.sum(jnp.where(mine_row, g_im, 0.0), axis=0, keepdims=True)
    far_fac_out[...] = jnp.where(line == 0, g_re, jnp.where(line == 1, g_im, 0.0))
    far_fac = copy_to(far_fac_out, far_fac_in, far_send.at[4, 0], far_recv.at[4, 0], (y_partner, rho))
    far_fac.start()
    pass_on(2)

    core_copy.wait_send()

    def rim_of(source, re, im):
        rim = jnp.concatenate(
            [
                source[QUARTERS - 1, CHUNK:WITH_RIM, :].astype(F32)[0:8],
                source[0, CHUNK:WITH_RIM, :].astype(F32)[8:16],
            ],
            axis=0,
        )
        return rotate(rim, re, im)

    for j in range(QUARTERS):
        own[j * CHUNK : (j + 1) * CHUNK, :] = rotate(back_in[j, 0:CHUNK, :], g_re, g_im)
    own[rows:total, :] = rim_of(back_in, g_re, g_im)
    big = total // 3

    @pl.loop(0, 3)
    def _(i):
        base = pl.multiple_of(i * big, 16)
        prod[pl.ds(base, big), :] = jnp.dot(own[pl.ds(base, big), :], matrix[10], preferred_element_type=F32)

    far_fac.wait_recv()
    far_re, far_im = far_fac_in[0:1, :], far_fac_in[1:2, :]
    y_mine = [taps[k, y_half, 3] for k in range(3)]
    y_theirs = [taps[k, 1 - y_half, 3] for k in range(3)]
    for e in (0, 1, 3, 2):
        each(behind[e], lambda k, e=e: far(e, k).wait_recv())
        base = pl.multiple_of(behind[e] * CHUNK, CHUNK)
        theirs = jnp.dot(
            rotate(far_in[behind[e], 0:CHUNK, :], far_re, far_im), matrix[11], preferred_element_type=F32
        )
        spread(base, CHUNK, prod[pl.ds(base, CHUNK), :], theirs, y_mine, y_theirs)
    theirs = jnp.dot(rim_of(far_in, far_re, far_im), matrix[11], preferred_element_type=F32)
    spread(rows, 16, prod[rows:total, :], theirs, y_mine, y_theirs)
    close(total)
    sums = zeros()
    for j in range(QUARTERS):
        y = merge(j * CHUNK, CHUNK)
        own[j * CHUNK : (j + 1) * CHUNK, :] = y
        sums = tally(y.astype(F32), sums)
    send_sums(1, sums)
    for j in range(QUARTERS):
        y = own[j * CHUNK : (j + 1) * CHUNK, :].astype(F32)
        for part in range(2):
            image[part, :, j * CHUNK : (j + 1) * CHUNK] = y[:, part * beams : (part + 1) * beams].T.astype(
                BF16
            )
    out = pltpu.make_async_copy(image, merged_hbm, load_sem.at[0])
    out.start()
    g_re, g_im = take_sums(1)
    phase[0:1, :] = g_re
    phase[1:2, :] = g_im

    for s in range(2):
        for d in range(n_rng - 1):
            sums_copy(s, d, rho).wait_send()
            wide_copy(s, d, rho).wait_send()
        for e in range(1, QUARTERS):
            part_copy(s, e, quarter).wait_send()
    for e in range(1, QUARTERS):
        split(e, quarter).wait_send()
        fac(e, quarter).wait_send()
        each(quarter, lambda k, e=e: back(e, quarter, k).wait_send())
    for e in range(QUARTERS):
        each(behind[e], lambda k, e=e: far(e, k).wait_send())
    far_fac.wait_send()
    out.wait()


def solution(mesh):
    n_rng = mesh.shape["rng"]

    def on_device(image, stencil, interp_weights, range_taps):
        _, beams, rows = image.shape
        total = rows + 16
        cosines, sines = angle_tables(beams)
        hbm = pl.BlockSpec(memory_space=pltpu.HBM)
        vmem = pl.BlockSpec(memory_space=pltpu.VMEM)
        smem = pl.BlockSpec(memory_space=pltpu.SMEM)
        dma = pltpu.SemaphoreType.DMA
        return pl.pallas_call(
            functools.partial(kernel, n_rng),
            out_shape=(
                jax.ShapeDtypeStruct((2, beams, rows), BF16),
                jax.ShapeDtypeStruct((2, beams), F32),
            ),
            in_specs=[smem, smem, hbm, hbm, hbm],
            out_specs=(hbm, vmem),
            scratch_shapes=[
                pltpu.VMEM((2, beams, rows), BF16),
                pltpu.VMEM((SECTIONS * 4, TAPS, beams), jnp.int32),
                pltpu.VMEM((2, SECTIONS * 4, beams), F32),
                pltpu.VMEM((total, 2 * beams), BF16),
                pltpu.VMEM((total, 2 * beams), BF16),
                pltpu.VMEM((12, 2 * beams, 2 * beams), BF16),
                pltpu.VMEM((total + 8, 2 * beams), F32),
                pltpu.VMEM((total, 2 * beams), F32),
                pltpu.VMEM((total + 8, 2 * beams), F32),
                pltpu.VMEM((total, 2 * beams), F32),
                pltpu.VMEM((16, 2 * beams), BF16),
                pltpu.VMEM((2, 2, 16, 2 * beams), BF16),
                pltpu.VMEM((2, 8, beams), F32),
                pltpu.VMEM((2, n_rng, 8, beams), F32),
                pltpu.VMEM((QUARTERS, WITH_RIM, 2 * beams), BF16),
                pltpu.VMEM((QUARTERS, WITH_RIM, 2 * beams), BF16),
                pltpu.VMEM((2, 2 * WITH_RIM, 2 * beams), BF16),
                pltpu.VMEM((2, 2 * WITH_RIM, 2 * beams), F32),
                pltpu.VMEM((QUARTERS, WITH_RIM, 2 * beams), BF16),
                pltpu.VMEM((QUARTERS, WITH_RIM, 2 * beams), BF16),
                pltpu.VMEM((QUARTERS, WITH_RIM, 2 * beams), BF16),
                pltpu.VMEM((QUARTERS, WITH_RIM, 2 * beams), BF16),
                pltpu.VMEM((8, beams), F32),
                pltpu.VMEM((QUARTERS, 8, beams), F32),
                pltpu.VMEM((8, beams), F32),
                pltpu.VMEM((8, beams), F32),
                pltpu.VMEM((2, 24, beams // 2), F32),
                pltpu.VMEM((2, n_rng, 24, beams // 2), F32),
                pltpu.VMEM((2, 24, beams // 2), F32),
                pltpu.VMEM((2, QUARTERS, 24, beams // 2), F32),
                dma((3,)),
                dma((1,)),
                dma((1,)),
                dma((2, 2)),
                dma((2, 2)),
                dma((2, n_rng - 1)),
                dma((2, n_rng - 1)),
                dma((QUARTERS - 1,)),
                dma((QUARTERS - 1,)),
                dma((QUARTERS - 1, 3)),
                dma((QUARTERS - 1, 3)),
                dma((QUARTERS + 1, 3)),
                dma((QUARTERS + 1, 3)),
                dma((QUARTERS - 1,)),
                dma((QUARTERS - 1,)),
                dma((2, n_rng - 1)),
                dma((2, n_rng - 1)),
                dma((2, QUARTERS - 1)),
                dma((2, QUARTERS - 1)),
            ],
            compiler_params=pltpu.CompilerParams(
                collective_id=0, has_side_effects=True, vmem_limit_bytes=67043328
            ),
        )(
            interp_weights,
            range_taps.transpose(2, 1, 0),
            image,
            stencil.transpose(0, 1, 2, 4, 3).reshape(SECTIONS * 4, TAPS, beams),
            jnp.asarray(np.stack([cosines, sines])),
        )

    return jax.shard_map(
        on_device,
        mesh=mesh,
        in_specs=(P(None, "sub", "rng"), P(), P(), P()),
        out_specs=(P(None, "sub", "rng"), P(None, "sub")),
        check_vma=False,
    )
```

```python
import functools

import jax
import jax.numpy as jnp
import numpy as np
from jax import lax
from jax.experimental import pallas as pl
from jax.experimental.pallas import tpu as pltpu
from jax.sharding import PartitionSpec as P

SECTIONS = 4
TAPS = 4
EPS = 1e-6
QUARTERS = 4
CHUNK = 128
WITH_RIM = CHUNK + 16
PARTS = ((0, CHUNK // 2), (CHUNK // 2, CHUNK // 2), (CHUNK, 16))
RIM = 2
MESH = pl.DeviceIdType.MESH
F32 = jnp.float32
BF16 = jnp.bfloat16


def angle_tables(beams):
    rows = []
    for s in range(SECTIONS):
        for h in range(2):
            for c in range(2):
                pos = np.float32(h * beams) + np.arange(beams, dtype=np.float32) + np.float32(0.5)
                rows.append(np.float32(2 * c - 1) * pos * np.float32(0.37 + 0.11 * s))
    psi = np.stack(rows).astype(np.float64)
    return np.cos(psi).astype(np.float32), np.sin(psi).astype(np.float32)


def kernel(
    n_rng,
    weights,
    taps,
    image_hbm,
    stencil_hbm,
    trig_hbm,
    merged_hbm,
    phase,
    image,
    stencil,
    trig,
    own,
    got,
    matrix,
    acc0,
    acc1,
    acc2,
    prod,
    edge_out,
    edge_in,
    sums_out,
    sums_in,
    split_out,
    split_in,
    stacked,
    terms,
    middle_y,
    back_out,
    back_in,
    far_in,
    fac_out,
    fac_in,
    far_fac_out,
    far_fac_in,
    wide_out,
    wide_in,
    part_out,
    part_in,
    load_sem,
    core_send,
    core_recv,
    edge_send,
    edge_recv,
    sums_send,
    sums_recv,
    split_send,
    split_recv,
    back_send,
    back_recv,
    far_send,
    far_recv,
    fac_send,
    fac_recv,
    wide_send,
    wide_recv,
    part_send,
    part_recv,
):
    sub = lax.axis_index("sub")
    rho = lax.axis_index("rng")
    beams = image.shape[1]
    rows = image.shape[2]
    total = rows + 16
    width = 2 * beams
    quarter = lax.rem(sub // 2, QUARTERS)
    core_half = lax.rem(sub, 2)
    y_half = lax.rem(sub // 8, 2)
    core_partner = sub + 1 - 2 * core_half
    y_partner = sub + 8 * (1 - 2 * y_half)
    ahead = [lax.rem(quarter + e, QUARTERS) for e in range(QUARTERS)]
    behind = [lax.rem(quarter + QUARTERS - e, QUARTERS) for e in range(QUARTERS)]
    peers = [lax.rem(rho + d, n_rng) for d in range(1, n_rng)]

    def at_quarter(other):
        return sub + 2 * (other - quarter)

    barrier = pltpu.get_barrier_semaphore()
    for other in (core_partner, y_partner, *[at_quarter(ahead[e]) for e in range(1, QUARTERS)]):
        pl.semaphore_signal(barrier, inc=1, device_id=(other, rho), device_id_type=MESH)
    for peer in peers:
        pl.semaphore_signal(barrier, inc=1, device_id=(sub, peer), device_id_type=MESH)
    below, above = lax.rem(rho + n_rng - 1, n_rng), lax.rem(rho + 1, n_rng)
    for peer in (below, above):
        pl.semaphore_signal(barrier, inc=1, device_id=(core_partner, peer), device_id_type=MESH)

    loads = [
        pltpu.make_async_copy(image_hbm, image, load_sem.at[0]),
        pltpu.make_async_copy(stencil_hbm, stencil, load_sem.at[1]),
        pltpu.make_async_copy(trig_hbm, trig, load_sem.at[2]),
    ]
    for load in loads:
        load.start()

    def build(slot, s, half, child):
        row = s * 4 + half * 2 + child
        shift = lax.broadcasted_iota(jnp.int32, (beams, beams), 0) - stencil[row, 0:1, :]
        cos_row = trig[0, pl.ds(row, 1), :]
        sin_row = trig[1, pl.ds(row, 1), :]
        real = jnp.zeros((beams, beams), F32)
        imag = jnp.zeros((beams, beams), F32)
        for t in range(TAPS):
            hit = shift == t
            real = jnp.where(hit, cos_row * weights[s, t], real)
            imag = jnp.where(hit, sin_row * weights[s, t], imag)
        matrix[slot, 0:beams, 0:beams] = real.astype(BF16)
        matrix[slot, 0:beams, beams:width] = imag.astype(BF16)
        matrix[slot, beams:width, 0:beams] = (-imag).astype(BF16)
        matrix[slot, beams:width, beams:width] = real.astype(BF16)

    def copy_to(src, dst, send, recv, target):
        return pltpu.make_async_remote_copy(
            src_ref=src, dst_ref=dst, send_sem=send, recv_sem=recv, device_id=target, device_id_type=MESH
        )

    for load in loads:
        load.wait()
    for j in range(rows // CHUNK):
        for part in range(2):
            block = image[part, :, j * CHUNK : (j + 1) * CHUNK].astype(F32)
            own[j * CHUNK : (j + 1) * CHUNK, part * beams : (part + 1) * beams] = block.T.astype(BF16)
    low_edge = own[0:16, :].astype(F32)
    high_edge = own[rows - 16 : rows, :].astype(F32)
    edge_out[...] = jnp.concatenate([low_edge[0:8], high_edge[8:16]], axis=0).astype(BF16)

    pl.semaphore_wait(barrier, 1 + 1 + QUARTERS - 1 + n_rng - 1 + 2)

    core_copy = copy_to(
        own.at[pl.ds(0, rows)], got.at[pl.ds(0, rows)], core_send.at[0], core_recv.at[0], (core_partner, rho)
    )

    def edge(whose, side):
        return copy_to(
            edge_out,
            edge_in.at[whose, side],
            edge_send.at[whose, side],
            edge_recv.at[whose, side],
            (core_partner if whose else sub, above if side == 0 else below),
        )

    for whose in range(2):
        for side in range(2):
            edge(whose, side).start()
    core_copy.start()
    build(0, 0, core_half, core_half)
    build(1, 0, core_half, 1 - core_half)

    row_id = lax.broadcasted_iota(jnp.int32, (16, width), 0)
    one = jnp.float32(1.0)
    spot = rho * QUARTERS + quarter
    low = jnp.where(rho < n_rng - 1, one, 0.0)
    high = jnp.where(rho > 0, one, 0.0)
    mask = jnp.where(row_id < 8, low, high)
    low = jnp.where(spot < n_rng * QUARTERS - 1, one, 0.0)
    high = jnp.where(spot > 0, one, 0.0)
    chunk_mask = jnp.where(row_id < 8, low, high)

    def rotate(value, g_re, g_im):
        value = value.astype(F32)
        real, imag = value[:, :beams], value[:, beams:]
        return jnp.concatenate(
            [(real * g_re - imag * g_im).astype(BF16), (real * g_im + imag * g_re).astype(BF16)], axis=1
        )

    def factors(re, im, power):
        scale = 1.0 / jnp.sqrt(power + EPS)
        return re * scale, -(im * scale)

    def tally(y, sums):
        real, imag = y[:, :beams], y[:, beams:]
        real_next, imag_next = pltpu.roll(real, beams - 1, 1), pltpu.roll(imag, beams - 1, 1)
        size = real.shape[0]
        products = (
            real * real_next + imag * imag_next,
            real * imag_next - imag * real_next,
            (real * real + imag * imag) * (real_next * real_next + imag_next * imag_next),
        )
        return [a + jnp.sum(p.reshape(size // 8, 8, beams), axis=0) for a, p in zip(sums, products)]

    def zeros():
        return [jnp.zeros((8, beams), F32) for _ in range(3)]

    def spread(base, size, mine, theirs, taps_mine, taps_theirs):
        acc0[pl.ds(base + 8, size), :] = taps_mine[0] * mine + taps_theirs[0] * theirs
        acc1[pl.ds(base, size), :] = taps_mine[1] * mine + taps_theirs[1] * theirs
        acc2[pl.ds(base, size), :] = taps_mine[2] * mine + taps_theirs[2] * theirs

    def close(length):
        acc0[0:8, :] = acc0[length : length + 8, :]
        acc2[length : length + 8, :] = acc2[0:8, :]

    def merge(base, size):
        lower = acc0[base : base + size + 8, :][7 : 7 + size]
        upper = acc2[base : base + size + 8, :][1 : 1 + size]
        return (acc1[base : base + size, :] + lower + upper).astype(BF16)

    line = lax.broadcasted_iota(jnp.int32, (8, beams), 0)

    def sums_copy(s, d, slot):
        return copy_to(
            sums_out.at[s], sums_in.at[s, slot], sums_send.at[s, d], sums_recv.at[s, d], (sub, peers[d])
        )

    def send_sums(s, sums):
        packed = jnp.zeros((8, beams), F32)
        for k in range(3):
            packed = jnp.where(line == k, jnp.sum(sums[k], axis=0, keepdims=True), packed)
        sums_out[s] = packed
        sums_in[s, rho] = packed
        for d in range(n_rng - 1):
            sums_copy(s, d, rho).start()

    def take_sums(s):
        for d in range(n_rng - 1):
            sums_copy(s, d, peers[n_rng - 2 - d]).wait_recv()
        full = sums_in[s, 0]
        for other in range(1, n_rng):
            full = full + sums_in[s, other]
        return factors(full[0:1], full[1:2], full[2:3])

    half_rows = rows // 2

    @pl.loop(0, 2)
    def _(i):
        base = pl.multiple_of(i * half_rows, 16)
        prod[pl.ds(base, half_rows), :] = jnp.dot(
            own[pl.ds(base, half_rows), :], matrix[0], preferred_element_type=F32
        )

    core_mine = [taps[k, core_half, 0] for k in range(3)]
    core_theirs = [taps[k, 1 - core_half, 0] for k in range(3)]
    core_copy.wait_recv()

    @pl.loop(0, 2)
    def _(i):
        base = pl.multiple_of(i * half_rows, 16)
        theirs = jnp.dot(got[pl.ds(base, half_rows), :], matrix[1], preferred_element_type=F32)
        spread(base, half_rows, prod[pl.ds(base, half_rows), :], theirs, core_mine, core_theirs)

    sums = zeros()

    def settle(j, sums):
        y = merge(j * CHUNK, CHUNK)
        split_out[j, 0:CHUNK, :] = y
        y = y.astype(F32)
        prod[j * CHUNK : j * CHUNK + 8, :] = y[0:8]
        prod[(j + 1) * CHUNK - 8 : (j + 1) * CHUNK, :] = y[CHUNK - 8 : CHUNK]
        return tally(y, sums)

    for j in range(1, QUARTERS - 1):
        sums = settle(j, sums)
    rims = []
    for whose in range(2):
        edge(whose, 0).wait()
        edge(whose, 1).wait()
        halo = jnp.concatenate(
            [edge_in[whose, 1].astype(F32)[0:8], edge_in[whose, 0].astype(F32)[8:16]], axis=0
        )
        rims.append(
            jnp.dot((halo * mask).astype(BF16), matrix[whose], preferred_element_type=F32)
        )
    spread(rows, 16, rims[0], rims[1], core_mine, core_theirs)
    close(total)
    for j in (0, QUARTERS - 1):
        sums = settle(j, sums)
    send_sums(0, sums)
    prod[rows:total, :] = merge(rows, 16).astype(F32) * mask
    for j in range(QUARTERS):
        after = (j + 1) * CHUNK
        before = (j * CHUNK - 8) % total
        split_out[j, CHUNK:WITH_RIM, :] = jnp.concatenate(
            [prod[after : after + 8, :], prod[before : before + 8, :]], axis=0
        ).astype(BF16)

    def split(e, slot):
        return copy_to(
            split_out.at[ahead[e]],
            split_in.at[slot],
            split_send.at[e - 1],
            split_recv.at[e - 1],
            (at_quarter(ahead[e]), rho),
        )

    def fac(e, slot):
        return copy_to(
            fac_out, fac_in.at[slot], fac_send.at[e - 1], fac_recv.at[e - 1], (at_quarter(ahead[e]), rho)
        )

    split(2, quarter).start()
    split(1, quarter).start()
    split_in[quarter] = split_out[quarter]
    g_re, g_im = take_sums(0)
    packed = jnp.where(line == 0, g_re, jnp.where(line == 1, g_im, 0.0))
    fac_out[...] = packed
    fac_in[quarter] = packed
    for e in (1, 3, 2):
        fac(e, quarter).start()
    split(3, quarter).start()

    for half in range(2):
        for child in range(2):
            build(2 + half * 2 + child, 1, half, child)
            build(6 + half * 2 + child, 2, half, child)
    build(10, 3, y_half, y_half)
    build(11, 3, y_half, 1 - y_half)

    def wide_copy(t, d, slot):
        return copy_to(
            wide_out.at[t], wide_in.at[t, slot], wide_send.at[t, d], wide_recv.at[t, d], (sub, peers[d])
        )

    def part_copy(t, e, slot):
        return copy_to(
            part_out.at[t],
            part_in.at[t, slot],
            part_send.at[t, e - 1],
            part_recv.at[t, e - 1],
            (at_quarter(ahead[e]), rho),
        )

    lanes = beams // 2
    tall = lax.broadcasted_iota(jnp.int32, (24, lanes), 0)

    def cross(t, target):
        s = t + 1
        packed = jnp.zeros((24, lanes), F32)
        for half in range(2):
            for child in range(2):
                terms[child] = jnp.dot(
                    stacked[child], matrix[2 + 4 * t + half * 2 + child], preferred_element_type=F32
                )
            for pair in range(2):
                block = 2 * pair + half if t == 0 else 2 * half + pair
                at = pair * WITH_RIM
                spread(
                    0,
                    WITH_RIM,
                    terms[0, at : at + WITH_RIM, :],
                    terms[1, at : at + WITH_RIM, :],
                    [taps[k, 0, s] for k in range(3)],
                    [taps[k, 1, s] for k in range(3)],
                )
                close(WITH_RIM)
                y = merge(0, CHUNK)
                target[block, 0:CHUNK, :] = y
                sums = tally(y.astype(F32), zeros())
                target[block, CHUNK:WITH_RIM, :] = (merge(CHUNK, 16).astype(F32) * chunk_mask).astype(BF16)
                for k in range(3):
                    value = jnp.sum(sums[k], axis=0, keepdims=True)
                    for side in range(2):
                        packed = jnp.where(
                            tall == k * 8 + side * 4 + block,
                            value[:, side * lanes : (side + 1) * lanes],
                            packed,
                        )
        wide_out[t] = packed
        wide_in[t, rho] = packed
        for d in range(n_rng - 1):
            wide_copy(t, d, rho).start()

    def narrow(t):
        for d in range(n_rng - 1):
            wide_copy(t, d, peers[n_rng - 2 - d]).wait_recv()
        full = wide_in[t, 0]
        for other in range(1, n_rng):
            full = full + wide_in[t, other]
        part_out[t] = full
        part_in[t, quarter] = full
        for e in (2, 1, 3):
            part_copy(t, e, quarter).start()

    def finish(t):
        for e in (1, 3, 2):
            part_copy(t, e, behind[e]).wait_recv()
        full = part_in[t, 0]
        for other in range(1, QUARTERS):
            full = full + part_in[t, other]
        whole = [jnp.concatenate([full[k : k + 4], full[k + 4 : k + 8]], axis=1) for k in (0, 8, 16)]
        return factors(*whole)

    for e in (0, 2, 1, 3):
        block = behind[e]
        if e > 0:
            fac(e, block).wait_recv()
            split(e, block).wait_recv()
        base = pl.multiple_of(block // 2 * WITH_RIM, 16)
        stacked[lax.rem(block, 2), pl.ds(base, WITH_RIM), :] = rotate(
            split_in[block], fac_in[block, 0:1, :], fac_in[block, 1:2, :]
        )
    cross(0, middle_y)
    narrow(0)
    g_re, g_im = finish(0)

    for block in range(QUARTERS):
        stacked[block // 2, (block % 2) * WITH_RIM : (block % 2 + 1) * WITH_RIM, :] = rotate(
            middle_y[block], g_re[block : block + 1], g_im[block : block + 1]
        )
    cross(1, back_out)

    def ends(slot):
        return lax.rem(slot, QUARTERS - 1) == 0

    def each(slot, action):
        pl.when(ends(slot))(lambda: action(RIM))
        action(0)
        action(1)

    def back(e, slot, k):
        rows_k = pl.ds(*PARTS[k])
        return copy_to(
            back_out.at[ahead[e], rows_k],
            back_in.at[slot, rows_k],
            back_send.at[e - 1, k],
            back_recv.at[e - 1, k],
            (at_quarter(ahead[e]), rho),
        )

    def far(e, k):
        rows_k = pl.ds(*PARTS[k])
        return copy_to(
            back_in.at[behind[e], rows_k],
            far_in.at[behind[e], rows_k],
            far_send.at[e, k],
            far_recv.at[e, k],
            (y_partner, rho),
        )

    def pass_on(e):
        def action(k):
            back(e, behind[e], k).wait_recv()
            far(e, k).start()

        each(behind[e], action)

    back_in[quarter] = back_out[quarter]
    for e in (1, 3):
        each(quarter, lambda k, e=e: back(e, quarter, k).start())
    each(quarter, lambda k: far(0, k).start())
    narrow(1)
    each(quarter, lambda k: back(2, quarter, k).start())
    for e in (1, 3):
        pass_on(e)
    g_re, g_im = finish(1)
    mine_row = lax.broadcasted_iota(jnp.int32, (4, beams), 0) == quarter
    g_re = jnp.sum(jnp.where(mine_row, g_re, 0.0), axis=0, keepdims=True)
    g_im = jnp.sum(jnp.where(mine_row, g_im, 0.0), axis=0, keepdims=True)
    far_fac_out[...] = jnp.where(line == 0, g_re, jnp.where(line == 1, g_im, 0.0))
    far_fac = copy_to(far_fac_out, far_fac_in, far_send.at[4, 0], far_recv.at[4, 0], (y_partner, rho))
    far_fac.start()
    pass_on(2)

    core_copy.wait_send()

    def rim_of(source, re, im):
        rim = jnp.concatenate(
            [
                source[QUARTERS - 1, CHUNK:WITH_RIM, :].astype(F32)[0:8],
                source[0, CHUNK:WITH_RIM, :].astype(F32)[8:16],
            ],
            axis=0,
        )
        return rotate(rim, re, im)

    for j in range(QUARTERS):
        own[j * CHUNK : (j + 1) * CHUNK, :] = rotate(back_in[j, 0:CHUNK, :], g_re, g_im)
    own[rows:total, :] = rim_of(back_in, g_re, g_im)
    big = total // 3

    @pl.loop(0, 3)
    def _(i):
        base = pl.multiple_of(i * big, 16)
        prod[pl.ds(base, big), :] = jnp.dot(own[pl.ds(base, big), :], matrix[10], preferred_element_type=F32)

    far_fac.wait_recv()
    far_re, far_im = far_fac_in[0:1, :], far_fac_in[1:2, :]
    y_mine = [taps[k, y_half, 3] for k in range(3)]
    y_theirs = [taps[k, 1 - y_half, 3] for k in range(3)]
    for e in (0, 1, 3, 2):
        each(behind[e], lambda k, e=e: far(e, k).wait_recv())
        base = pl.multiple_of(behind[e] * CHUNK, CHUNK)
        theirs = jnp.dot(
            rotate(far_in[behind[e], 0:CHUNK, :], far_re, far_im), matrix[11], preferred_element_type=F32
        )
        spread(base, CHUNK, prod[pl.ds(base, CHUNK), :], theirs, y_mine, y_theirs)
    theirs = jnp.dot(rim_of(far_in, far_re, far_im), matrix[11], preferred_element_type=F32)
    spread(rows, 16, prod[rows:total, :], theirs, y_mine, y_theirs)
    close(total)
    sums = zeros()
    for j in range(QUARTERS):
        y = merge(j * CHUNK, CHUNK)
        own[j * CHUNK : (j + 1) * CHUNK, :] = y
        sums = tally(y.astype(F32), sums)
    send_sums(1, sums)
    for j in range(QUARTERS):
        y = own[j * CHUNK : (j + 1) * CHUNK, :].astype(F32)
        for part in range(2):
            image[part, :, j * CHUNK : (j + 1) * CHUNK] = y[:, part * beams : (part + 1) * beams].T.astype(
                BF16
            )
    out = pltpu.make_async_copy(image, merged_hbm, load_sem.at[0])
    out.start()
    g_re, g_im = take_sums(1)
    phase[0:1, :] = g_re
    phase[1:2, :] = g_im

    for s in range(2):
        for d in range(n_rng - 1):
            sums_copy(s, d, rho).wait_send()
            wide_copy(s, d, rho).wait_send()
        for e in range(1, QUARTERS):
            part_copy(s, e, quarter).wait_send()
    for e in range(1, QUARTERS):
        split(e, quarter).wait_send()
        fac(e, quarter).wait_send()
        each(quarter, lambda k, e=e: back(e, quarter, k).wait_send())
    for e in range(QUARTERS):
        each(behind[e], lambda k, e=e: far(e, k).wait_send())
    far_fac.wait_send()
    out.wait()


def solution(mesh):
    n_rng = mesh.shape["rng"]

    def on_device(image, stencil, interp_weights, range_taps):
        _, beams, rows = image.shape
        total = rows + 16
        cosines, sines = angle_tables(beams)
        hbm = pl.BlockSpec(memory_space=pltpu.HBM)
        vmem = pl.BlockSpec(memory_space=pltpu.VMEM)
        smem = pl.BlockSpec(memory_space=pltpu.SMEM)
        dma = pltpu.SemaphoreType.DMA
        return pl.pallas_call(
            functools.partial(kernel, n_rng),
            out_shape=(
                jax.ShapeDtypeStruct((2, beams, rows), BF16),
                jax.ShapeDtypeStruct((2, beams), F32),
            ),
            in_specs=[smem, smem, hbm, hbm, hbm],
            out_specs=(hbm, vmem),
            scratch_shapes=[
                pltpu.VMEM((2, beams, rows), BF16),
                pltpu.VMEM((SECTIONS * 4, TAPS, beams), jnp.int32),
                pltpu.VMEM((2, SECTIONS * 4, beams), F32),
                pltpu.VMEM((total, 2 * beams), BF16),
                pltpu.VMEM((total, 2 * beams), BF16),
                pltpu.VMEM((12, 2 * beams, 2 * beams), BF16),
                pltpu.VMEM((total + 8, 2 * beams), F32),
                pltpu.VMEM((total, 2 * beams), F32),
                pltpu.VMEM((total + 8, 2 * beams), F32),
                pltpu.VMEM((total, 2 * beams), F32),
                pltpu.VMEM((16, 2 * beams), BF16),
                pltpu.VMEM((2, 2, 16, 2 * beams), BF16),
                pltpu.VMEM((2, 8, beams), F32),
                pltpu.VMEM((2, n_rng, 8, beams), F32),
                pltpu.VMEM((QUARTERS, WITH_RIM, 2 * beams), BF16),
                pltpu.VMEM((QUARTERS, WITH_RIM, 2 * beams), BF16),
                pltpu.VMEM((2, 2 * WITH_RIM, 2 * beams), BF16),
                pltpu.VMEM((2, 2 * WITH_RIM, 2 * beams), F32),
                pltpu.VMEM((QUARTERS, WITH_RIM, 2 * beams), BF16),
                pltpu.VMEM((QUARTERS, WITH_RIM, 2 * beams), BF16),
                pltpu.VMEM((QUARTERS, WITH_RIM, 2 * beams), BF16),
                pltpu.VMEM((QUARTERS, WITH_RIM, 2 * beams), BF16),
                pltpu.VMEM((8, beams), F32),
                pltpu.VMEM((QUARTERS, 8, beams), F32),
                pltpu.VMEM((8, beams), F32),
                pltpu.VMEM((8, beams), F32),
                pltpu.VMEM((2, 24, beams // 2), F32),
                pltpu.VMEM((2, n_rng, 24, beams // 2), F32),
                pltpu.VMEM((2, 24, beams // 2), F32),
                pltpu.VMEM((2, QUARTERS, 24, beams // 2), F32),
                dma((3,)),
                dma((1,)),
                dma((1,)),
                dma((2, 2)),
                dma((2, 2)),
                dma((2, n_rng - 1)),
                dma((2, n_rng - 1)),
                dma((QUARTERS - 1,)),
                dma((QUARTERS - 1,)),
                dma((QUARTERS - 1, 3)),
                dma((QUARTERS - 1, 3)),
                dma((QUARTERS + 1, 3)),
                dma((QUARTERS + 1, 3)),
                dma((QUARTERS - 1,)),
                dma((QUARTERS - 1,)),
                dma((2, n_rng - 1)),
                dma((2, n_rng - 1)),
                dma((2, QUARTERS - 1)),
                dma((2, QUARTERS - 1)),
            ],
            compiler_params=pltpu.CompilerParams(
                collective_id=0, has_side_effects=True, vmem_limit_bytes=67043328
            ),
        )(
            interp_weights,
            range_taps.transpose(2, 1, 0),
            image,
            stencil.transpose(0, 1, 2, 4, 3).reshape(SECTIONS * 4, TAPS, beams),
            jnp.asarray(np.stack([cosines, sines])),
        )

    return jax.shard_map(
        on_device,
        mesh=mesh,
        in_specs=(P(None, "sub", "rng"), P(), P(), P()),
        out_specs=(P(None, "sub", "rng"), P(None, "sub")),
        check_vma=False,
    )
```
